32 devices in a mesh: dp: 1 (over z), cp: 4 (over y), tp: 8 (over x, core).
Axes of the slice: x: 4, y: 4, z: 1, core: 2. Of those that a mesh axis runs over, the one named last changes fastest.
The devices are a block of a 4x4x8 slice.
Arguments:
- hidden_in: bfloat16 [6144, 2048], P(('dp', 'cp', 'tp'))
- w_query: bfloat16 [2048, 16, 128], P(None, 'tp')
- w_key: bfloat16 [2048, 16, 128], P(None, 'tp')
- w_value: bfloat16 [2048, 16, 128], P(None, 'tp')
- w_out: bfloat16 [16, 128, 2048], P('tp')
- expert_idx: int32 [6144, 6], P(('dp', 'cp', 'tp'))
- gate_vals: float32 [6144, 6], P(('dp', 'cp', 'tp'))
- w_gate: bfloat16 [64, 2048, 1408], P(('cp', 'tp'))
- w_up: bfloat16 [64, 2048, 1408], P(('cp', 'tp'))
- w_down: bfloat16 [64, 1408, 2048], P(('cp', 'tp'))
Outputs:
- output: bfloat16 [6144, 2048], P(('dp', 'cp', 'tp'))
All inputs are finite; a program needn't handle non-finite values.
Results may differ from the reference program's by a relative error of at most 0.014792.
Values are sent between devices in bfloat16 or wider.
A program may use at most 768 MiB of HBM per device.

```python
import jax
import jax.numpy as jnp
from jax import lax

HIDDEN = 2048
FFN_DIM = 1408
Q_HEADS = 16
KV_HEADS = 16
HEAD_DIM = 128
EXPERTS = 64
TOP_K = 6
DEV_LIMIT = 3
TOK_DEV = 192
CP_DEVS = 4
TP_DEVS = 8

GROUP_DEVS = CP_DEVS * TP_DEVS
SEQ_LEN = TOK_DEV * GROUP_DEVS
BLOCK_ROWS = SEQ_LEN // CP_DEVS
CHUNK_ROWS = BLOCK_ROWS // 2
QUERY_ROWS = min(64, SEQ_LEN)
PER_EXPERT = SEQ_LEN * TOP_K // EXPERTS


def draw_routing(rand_key):
    local_exp = EXPERTS // GROUP_DEVS
    per_dev = TOK_DEV * DEV_LIMIT // GROUP_DEVS
    per_tok = TOP_K // DEV_LIMIT
    capacity = TOK_DEV * TOP_K // EXPERTS
    key_dev, key_loc, key_tok = jax.random.split(rand_key, 3)
    dev_perm = jax.vmap(lambda sub_key: jax.random.permutation(sub_key, GROUP_DEVS))(jax.random.split(key_dev, GROUP_DEVS))
    loc_perm = jax.vmap(lambda sub_key: jax.random.permutation(sub_key, local_exp))(jax.random.split(key_loc, GROUP_DEVS * GROUP_DEVS)).reshape(GROUP_DEVS, GROUP_DEVS, local_exp)
    tok_perm = jax.vmap(lambda sub_key: jax.random.permutation(sub_key, TOK_DEV))(jax.random.split(key_tok, GROUP_DEVS))
    place_ids = jnp.arange(TOK_DEV)[:, None] + TOK_DEV * jnp.arange(DEV_LIMIT)[None, :]
    dev_block = place_ids // per_dev
    dev_rank = place_ids - dev_block * per_dev
    target = dev_perm[:, dev_block]
    sub_place = dev_rank[:, :, None] + per_dev * jnp.arange(per_tok)[None, None, :]
    loc_block = sub_place // capacity
    src_ids = jnp.arange(GROUP_DEVS)[:, None, None, None]
    local_ids = loc_perm[src_ids, target[:, :, :, None], loc_block[None]]
    expert = target[:, :, :, None] * local_exp + local_ids
    expert = expert.reshape(GROUP_DEVS, TOK_DEV, TOP_K)
    expert = jnp.take_along_axis(expert, tok_perm[:, :, None], axis=1)
    return expert.reshape(SEQ_LEN, TOP_K).astype(jnp.int32)


def setup_inputs(seed: int = 0, part: int = 0) -> dict:
    base_key = jax.random.key(seed)
    shared = jax.random.split(base_key, 7)
    own = jax.random.split(jax.random.fold_in(base_key, part), 3)
    q_scale = 2.0 * HIDDEN ** -0.5
    hidden_in = jax.random.normal(own[0], (SEQ_LEN, HIDDEN), jnp.float32)
    w_query = q_scale * jax.random.normal(shared[0], (HIDDEN, Q_HEADS, HEAD_DIM), jnp.float32)
    w_key = q_scale * jax.random.normal(shared[1], (HIDDEN, KV_HEADS, HEAD_DIM), jnp.float32)
    w_value = HIDDEN ** -0.5 * jax.random.normal(shared[2], (HIDDEN, KV_HEADS, HEAD_DIM), jnp.float32)
    w_out = (Q_HEADS * HEAD_DIM) ** -0.5 * jax.random.normal(shared[3], (Q_HEADS, HEAD_DIM, HIDDEN), jnp.float32)
    w_gate = HIDDEN ** -0.5 * jax.random.normal(shared[4], (EXPERTS, HIDDEN, FFN_DIM), jnp.float32)
    w_up = HIDDEN ** -0.5 * jax.random.normal(shared[5], (EXPERTS, HIDDEN, FFN_DIM), jnp.float32)
    w_down = FFN_DIM ** -0.5 * jax.random.normal(shared[6], (EXPERTS, FFN_DIM, HIDDEN), jnp.float32)
    expert_idx = draw_routing(own[1])
    gate_vals = jax.random.uniform(own[2], (SEQ_LEN, TOP_K), jnp.float32, 0.2, 0.6)
    return dict(hidden_in=hidden_in.astype(jnp.bfloat16), w_query=w_query.astype(jnp.bfloat16), w_key=w_key.astype(jnp.bfloat16), w_value=w_value.astype(jnp.bfloat16), w_out=w_out.astype(jnp.bfloat16), expert_idx=expert_idx, gate_vals=gate_vals, w_gate=w_gate.astype(jnp.bfloat16), w_up=w_up.astype(jnp.bfloat16), w_down=w_down.astype(jnp.bfloat16))


def row_positions(row_ids):
    block_id = row_ids // BLOCK_ROWS
    offset_in = row_ids % BLOCK_ROWS
    return jnp.where(offset_in < CHUNK_ROWS, block_id * CHUNK_ROWS + offset_in, (2 * CP_DEVS - 1 - block_id) * CHUNK_ROWS + offset_in - CHUNK_ROWS)


def reference(hidden_in, w_query, w_key, w_value, w_out, expert_idx, gate_vals, w_gate, w_up, w_down):
    group_size = Q_HEADS // KV_HEADS
    position = row_positions(jnp.arange(SEQ_LEN))
    query_vecs = jnp.dot(hidden_in, w_query.reshape(HIDDEN, -1), preferred_element_type=jnp.float32).astype(jnp.bfloat16)
    key_vecs = jnp.dot(hidden_in, w_key.reshape(HIDDEN, -1), preferred_element_type=jnp.float32).astype(jnp.bfloat16)
    value_vecs = jnp.dot(hidden_in, w_value.reshape(HIDDEN, -1), preferred_element_type=jnp.float32).astype(jnp.bfloat16)
    query_vecs = query_vecs.astype(jnp.float32).reshape(SEQ_LEN // QUERY_ROWS, QUERY_ROWS, KV_HEADS, group_size, HEAD_DIM)
    key_vecs = key_vecs.astype(jnp.float32).reshape(SEQ_LEN, KV_HEADS, HEAD_DIM)
    value_vecs = value_vecs.astype(jnp.float32).reshape(SEQ_LEN, KV_HEADS, HEAD_DIM)
    score_scale = HEAD_DIM ** -0.5

    def attend(operands):
        q_blk, q_place = operands
        scores = jnp.einsum('qgrd,kgd->qgrk', q_blk, key_vecs) * score_scale
        allowed = position[None, None, None, :] <= q_place[:, None, None, None]
        scores = jnp.where(allowed, scores, -1e30)
        attn_prob = jax.nn.softmax(scores, axis=-1)
        attn_out = jnp.einsum('qgrk,kgd->qgrd', attn_prob, value_vecs)
        return attn_out.reshape(QUERY_ROWS, Q_HEADS * HEAD_DIM).astype(jnp.bfloat16)

    attn_all = lax.map(attend, (query_vecs, position.reshape(-1, QUERY_ROWS))).reshape(SEQ_LEN, Q_HEADS * HEAD_DIM)
    proj_sum = jnp.dot(attn_all, w_out.reshape(-1, HIDDEN), preferred_element_type=jnp.float32)
    resid_f = (hidden_in.astype(jnp.float32) + proj_sum).astype(jnp.bfloat16).astype(jnp.float32)
    sort_order = jnp.argsort(expert_idx.reshape(-1), stable=True)
    tok_rows = (sort_order // TOP_K).reshape(EXPERTS, PER_EXPERT)

    def expert_fn(operands):
        row_ids, gate_w, up_w, down_w = operands
        rows_in = resid_f[row_ids]
        gate_act = jnp.dot(rows_in, gate_w.astype(jnp.float32), preferred_element_type=jnp.float32)
        up_act = jnp.dot(rows_in, up_w.astype(jnp.float32), preferred_element_type=jnp.float32)
        hidden_act = (jax.nn.silu(gate_act) * up_act).astype(jnp.bfloat16).astype(jnp.float32)
        return jnp.dot(hidden_act, down_w.astype(jnp.float32), preferred_element_type=jnp.float32).astype(jnp.bfloat16)

    expert_out = lax.map(expert_fn, (tok_rows, w_gate, w_up, w_down)).reshape(SEQ_LEN * TOP_K, HIDDEN)
    inverse = jnp.argsort(sort_order)
    per_choice = expert_out[inverse].reshape(SEQ_LEN, TOP_K, HIDDEN).astype(jnp.float32)
    moe_sum = jnp.sum(gate_vals[:, :, None] * per_choice, axis=1)
    return (resid_f + moe_sum).astype(jnp.bfloat16)
```

```python
import functools
import math
import jax
import jax.numpy as jnp
from jax import lax
from jax.experimental import pallas as pl
from jax.experimental.pallas import tpu as pltpu

LANES = 128
VMEM_BYTES = 66 * 1024 * 1024


CORES = 2


def spread_order(cp_devs, tp_devs):
    x_devs = tp_devs // CORES
    row, col = lax.axis_index('cp'), lax.axis_index('tp') // CORES
    core = lax.rem(lax.axis_index('tp'), CORES)
    hops = lambda d, n: min(d, n - d)
    chips = [(dx, dy) for dx in range(x_devs) for dy in range(cp_devs)]
    chips.sort(key=lambda o: (-(hops(o[0], x_devs) + hops(o[1], cp_devs)), abs(hops(o[0], x_devs) - hops(o[1], cp_devs)), (o[0] * 3 + o[1] * 5) % 4))
    for dc in range(CORES):
        for dx, dy in chips:
            if dx or dy or dc:
                yield lax.rem(row + dy, cp_devs) * tp_devs + lax.rem(col + dx, x_devs) * CORES + lax.rem(core + dc, CORES)


def moe_kernel(cp_devs, tp_devs, chunks, src_ref, pos_ref, gate_ref, h_ref, wg_ref, wu_ref, wd_ref, y_ref,
               send, recv, xbuf, wgu, wdv, act, wide, zsend, ret, w_sem, loc_sem, dsend_sem, drecv_sem, rsend_sem, rrecv_sem):
    n_dev = cp_devs * tp_devs
    local_exp = wg_ref.shape[0]
    tok_dev, sub = h_ref.shape[0], h_ref.shape[1]
    slots = send.shape[2]
    rows = n_dev * slots
    gu_tiles, dn_tiles = wgu.shape[1], wdv.shape[1]
    dn_cols = wdv.shape[3]
    top_k = gate_ref.shape[0] // tok_dev
    me = lax.axis_index('cp') * tp_devs + lax.axis_index('tp')

    def place(dev):
        return {'cp': dev // tp_devs, 'tp': lax.rem(dev, tp_devs)}

    barrier = pltpu.get_barrier_semaphore()

    def greet(p, carry):
        pl.semaphore_signal(barrier, inc=1, device_id=place(lax.rem(me + p, n_dev)), device_id_type=pl.DeviceIdType.MESH)
        return carry

    lax.fori_loop(1, n_dev, greet, 0)

    def gu_copy(e, j, half, ref):
        return pltpu.make_async_copy(ref.at[e, :, pl.ds(pl.multiple_of(j * LANES, LANES), LANES)],
                                     wgu.at[e, j, :, pl.ds(half * LANES, LANES)], w_sem.at[0, e])

    def dn_copy(e, j):
        return pltpu.make_async_copy(wd_ref.at[e, :, pl.ds(pl.multiple_of(j * dn_cols, dn_cols), dn_cols)], wdv.at[e, j], w_sem.at[1, e])

    for e in range(local_exp):
        @pl.loop(0, gu_tiles)
        def _(j):
            gu_copy(e, j, 0, wg_ref).start()
            gu_copy(e, j, 1, wu_ref).start()

        @pl.loop(0, dn_tiles)
        def _(j):
            dn_copy(e, j).start()

    def fill(dev, carry):
        for c in range(chunks):
            for s in range(slots):
                send[c, dev, s] = h_ref[src_ref[(c * n_dev + dev) * slots + s]]
        return carry

    lax.fori_loop(0, n_dev, fill, 0)
    pl.semaphore_wait(barrier, n_dev - 1)

    def dispatch(c, dev):
        return pltpu.make_async_remote_copy(src_ref=send.at[c, dev], dst_ref=recv.at[c, me], send_sem=dsend_sem.at[c], recv_sem=drecv_sem.at[c],
                                            device_id=place(dev), device_id_type=pl.DeviceIdType.MESH)

    def give_back(c, dev):
        return pltpu.make_async_remote_copy(src_ref=zsend.at[c, dev], dst_ref=ret.at[c, me], send_sem=rsend_sem.at[c], recv_sem=rrecv_sem.at[c],
                                            device_id=place(dev), device_id_type=pl.DeviceIdType.MESH)

    def all_of(copy, c, what):
        if what == 'start':
            for dev in spread_order(cp_devs, tp_devs):
                copy(c, dev).start()
            return
        far = pl.ds(0, n_dev - 1)
        if copy is dispatch:
            every = pltpu.make_async_remote_copy(src_ref=send.at[c, far], dst_ref=recv.at[c, far], send_sem=dsend_sem.at[c], recv_sem=drecv_sem.at[c],
                                                 device_id=place(lax.rem(me + 1, n_dev)), device_id_type=pl.DeviceIdType.MESH)
        else:
            every = pltpu.make_async_remote_copy(src_ref=zsend.at[c, far], dst_ref=ret.at[c, far], send_sem=rsend_sem.at[c], recv_sem=rrecv_sem.at[c],
                                                 device_id=place(lax.rem(me + 1, n_dev)), device_id_type=pl.DeviceIdType.MESH)
        getattr(every, what)()

    for c in range(chunks):
        all_of(dispatch, c, 'start')
        pltpu.make_async_copy(send.at[c, me], recv.at[c, me], loc_sem.at[c]).start()

    for c in range(chunks):
        pltpu.make_async_copy(send.at[c, me], recv.at[c, me], loc_sem.at[c]).wait()
        all_of(dispatch, c, 'wait_recv')

        @pl.loop(0, n_dev)
        def _(dev):
            for s in range(slots):
                wide[pl.ds(pl.multiple_of((dev * slots + s) * sub, sub), sub), :] = recv[c, dev, s].astype(jnp.float32)

        for q in range(sub):
            xbuf[:, q * LANES:(q + 1) * LANES] = wide[pl.ds(q, rows, stride=sub), :].astype(jnp.bfloat16)

        @pl.loop(0, local_exp)
        def _(e):
            if c == 0:
                pltpu.make_async_copy(wgu.at[e], wgu.at[e], w_sem.at[0, e]).wait()
                pltpu.make_async_copy(wdv.at[e], wdv.at[e], w_sem.at[1, e]).wait()

            @pl.loop(0, gu_tiles)
            def _(j):
                both = jnp.dot(xbuf[...], wgu[e, j], preferred_element_type=jnp.float32)
                gate, up = both[:, :LANES], both[:, LANES:]
                act[:, pl.ds(pl.multiple_of(j * LANES, LANES), LANES)] = (gate * jax.nn.sigmoid(gate) * up).astype(jnp.bfloat16)

            @pl.loop(0, dn_tiles)
            def _(j):
                z = jnp.dot(act[...], wdv[e, j], preferred_element_type=jnp.float32)
                for i in range(dn_cols // LANES):
                    wide[pl.ds(j * (dn_cols // LANES) + i, rows, stride=sub), :] = z[:, i * LANES:(i + 1) * LANES]

            @pl.loop(0, n_dev)
            def _(dev):
                for s in range(slots):
                    zsend[c, dev, e, s] = wide[pl.ds(pl.multiple_of((dev * slots + s) * sub, sub), sub), :].astype(jnp.bfloat16)

        all_of(give_back, c, 'start')
        pltpu.make_async_copy(zsend.at[c, me], ret.at[c, me], loc_sem.at[chunks + c]).start()

    for c in range(chunks):
        pltpu.make_async_copy(zsend.at[c, me], ret.at[c, me], loc_sem.at[chunks + c]).wait()
        all_of(give_back, c, 'wait_recv')
    for c in range(chunks):
        all_of(dispatch, c, 'wait_send')
        all_of(give_back, c, 'wait_send')

    @pl.loop(0, tok_dev)
    def _(t):
        total = jnp.zeros((sub, LANES), jnp.float32)
        for k in range(top_k):
            at = pos_ref[t * top_k + k]
            dev_at = at // (local_exp * slots)
            rest = lax.rem(at, local_exp * slots)
            c_at = dev_at // n_dev
            total += gate_ref[t * top_k + k] * ret[c_at, lax.rem(dev_at, n_dev), rest // slots, lax.rem(rest, slots)].astype(jnp.float32)
        y_ref[t] = (h_ref[t].astype(jnp.float32) + total).astype(jnp.bfloat16)


def routing_tables(expert_idx, local_exp, n_dev, chunks):
    tok_dev, top_k = expert_idx.shape
    per_dev = tok_dev * top_k // (n_dev * local_exp)
    slots = per_dev // chunks
    dev = expert_idx // local_exp
    devs = jnp.arange(n_dev)
    member = jnp.any(dev[:, :, None] == devs[None, None, :], axis=1)
    before = (jnp.arange(tok_dev)[:, None] > jnp.arange(tok_dev)[None, :]).astype(jnp.bfloat16)
    slot_all = jnp.dot(before, member.astype(jnp.bfloat16), preferred_element_type=jnp.float32).astype(jnp.int32)
    slot = jnp.sum(jnp.where(dev[:, :, None] == devs[None, None, :], slot_all[:, None, :], 0), axis=2)
    here = member[:, :, None] & (slot_all[:, :, None] == jnp.arange(per_dev)[None, None, :])
    src = jnp.sum(jnp.where(here, jnp.arange(tok_dev, dtype=jnp.int32)[:, None, None], 0), axis=0)
    src = src.reshape(n_dev, chunks, slots).transpose(1, 0, 2).reshape(-1)
    pos = (((slot // slots) * n_dev + dev) * local_exp + expert_idx % local_exp) * slots + slot % slots
    return src, pos.reshape(-1)


def moe(h_tiles, expert_idx, gate_vals, w_gate, w_up, w_down, cp_devs, tp_devs, chunks=2):
    tok_dev, sub, _ = h_tiles.shape
    hidden = sub * LANES
    local_exp, _, ffn = w_gate.shape
    top_k = expert_idx.shape[1]
    n_dev = cp_devs * tp_devs
    slots = tok_dev * top_k // (n_dev * local_exp) // chunks
    rows = n_dev * slots
    gu_tiles, dn_cols = ffn // LANES, 2 * LANES
    dn_tiles = hidden // dn_cols
    src, pos = routing_tables(expert_idx, local_exp, n_dev, chunks)
    bf16, f32 = jnp.bfloat16, jnp.float32
    flops = 6 * chunks * rows * local_exp * hidden * ffn
    out = pl.pallas_call(
        functools.partial(moe_kernel, cp_devs, tp_devs, chunks),
        out_shape=jax.ShapeDtypeStruct((tok_dev, sub, LANES), bf16),
        in_specs=[pl.BlockSpec(memory_space=pltpu.SMEM)] * 3 + [pl.BlockSpec(memory_space=pltpu.VMEM)] + [pl.BlockSpec(memory_space=pl.ANY)] * 3,
        out_specs=pl.BlockSpec(memory_space=pltpu.VMEM),
        scratch_shapes=[
            pltpu.VMEM((chunks, n_dev, slots, sub, LANES), bf16),
            pltpu.VMEM((chunks, n_dev, slots, sub, LANES), bf16),
            pltpu.VMEM((rows, hidden), bf16),
            pltpu.VMEM((local_exp, gu_tiles, hidden, 2 * LANES), bf16),
            pltpu.VMEM((local_exp, dn_tiles, ffn, dn_cols), bf16),
            pltpu.VMEM((rows, ffn), bf16),
            pltpu.VMEM((rows * sub, LANES), f32),
            pltpu.VMEM((chunks, n_dev, local_exp, slots, sub, LANES), bf16),
            pltpu.VMEM((chunks, n_dev, local_exp, slots, sub, LANES), bf16),
            pltpu.SemaphoreType.DMA((2, local_exp)),
            pltpu.SemaphoreType.DMA((2 * chunks,)),
            pltpu.SemaphoreType.DMA((chunks,)),
            pltpu.SemaphoreType.DMA((chunks,)),
            pltpu.SemaphoreType.DMA((chunks,)),
            pltpu.SemaphoreType.DMA((chunks,)),
        ],
        compiler_params=pltpu.CompilerParams(collective_id=0, has_side_effects=True, vmem_limit_bytes=67043328),
        cost_estimate=pl.CostEstimate(flops=flops, bytes_accessed=6 * local_exp * hidden * ffn, transcendentals=rows * ffn),
        name='moe_exchange',
    )(src, pos, gate_vals.reshape(-1), h_tiles, w_gate, w_up, w_down)
    return out.reshape(tok_dev, hidden)


RING = 4
BATCHES = (((0, 0, 0), (0, 0, 1), (0, 1, 0), (0, 1, 1)),
           ((1, 0, 0), (1, 1, 0), (3, 0, 0), (3, 1, 0)),
           ((1, 0, 1), (1, 1, 1), (3, 0, 1), (3, 1, 1)),
           ((2, 0, 0), (2, 0, 1), (2, 1, 0), (2, 1, 1)))
SEND_ORDER = ((1, 0), (3, 0), (1, 1), (3, 1), (2, 0), (2, 1))


def attention_kernel(cp_devs, tp_devs, hid_ref, w_ref, wo_ref, h_ref,
                     xg, stage, q_all, kv_all, o_st, og, o_rows, wo_all, wide, acc, m_run, l_run,
                     xs_sem, xr_sem, fs_sem, fr_sem, ys_sem, yq_sem, ykv_sem, ks_sem, kr_sem, ws_sem, wr_sem, wfs_sem, wfr_sem, os_sem, or_sem):
    row, tp = lax.axis_index('cp'), lax.axis_index('tp')
    col, core = tp // CORES, lax.rem(tp, CORES)
    x_devs = tp_devs // CORES
    n_dev = cp_devs * tp_devs
    n_half, half_rows, hidden = hid_ref.shape
    units = tp_devs * n_half
    half_units = units // 2
    half_cp = cp_devs // 2
    batch_units = len(BATCHES[0])
    n_heads_loc = stage.shape[1]
    wo_rows = wo_ref.shape[0]
    f32, bf16 = jnp.float32, jnp.bfloat16
    mesh_id = pl.DeviceIdType.MESH
    sibling = {'cp': row, 'tp': col * CORES + 1 - core}

    def remote(src, dst, send_sem, recv_sem, dev):
        return pltpu.make_async_remote_copy(src_ref=src, dst_ref=dst, send_sem=send_sem, recv_sem=recv_sem, device_id=dev, device_id_type=mesh_id)

    def beside(d):
        return {'cp': row, 'tp': lax.rem(col + d, x_devs) * CORES + core}

    barrier = pltpu.get_barrier_semaphore()

    def greet(p, carry):
        dev = lax.rem(row * tp_devs + tp + p, n_dev)
        pl.semaphore_signal(barrier, inc=1, device_id={'cp': dev // tp_devs, 'tp': lax.rem(dev, tp_devs)}, device_id_type=mesh_id)
        return carry

    lax.fori_loop(1, n_dev, greet, 0)
    xg[0, 0] = hid_ref[0]
    xg[0, 1] = hid_ref[1]
    wo_all[pl.ds(pl.multiple_of(tp * wo_rows, wo_rows), wo_rows), :] = wo_ref[...]
    pl.semaphore_wait(barrier, n_dev - 1)

    where = {och: (b, u) for b, batch in enumerate(BATCHES) for u, och in enumerate(batch)}

    def direct(d, h):
        o = x_devs - d
        b, u = where[(o, 0, h)]
        return remote(hid_ref.at[h], xg.at[b, u], xs_sem.at[d - 1, h], xr_sem.at[o - 1, h], beside(d))

    def handed(o, h):
        b, u = where[(o, 0, h)]
        b2, u2 = where[(o, 1, h)]
        src = hid_ref.at[h] if o == 0 else xg.at[b, u]
        return remote(src, xg.at[b2, u2], fs_sem.at[o, h], fr_sem.at[o, h], sibling)

    for h in range(n_half):
        handed(0, h).start()
    for d, h in SEND_ORDER:
        direct(d, h).start()

    def unit_of(o, c, h):
        return (lax.rem(col + o, x_devs) * CORES + lax.rem(core + c, CORES)) * n_half + h

    def exchange(b):
        for i in range(n_heads_loc):
            to_row = core * n_heads_loc + i
            own = to_row == row
            for u, (o, c, h) in enumerate(BATCHES[b]):
                unit = unit_of(o, c, h)
                for kind, src, dst, sem in ((0, stage.at[b, i, u, 0], q_all.at[lax.rem(row, half_cp), unit], yq_sem),
                                            (1, stage.at[b, i, u, pl.ds(1, 2)], kv_all.at[row, unit], ykv_sem)):
                    got = sem.at[lax.rem(row, half_cp), b]

                    @pl.when(own)
                    def _():
                        pltpu.make_async_copy(src, dst, got).start()

                    @pl.when(jnp.logical_not(own))
                    def _():
                        remote(src, dst, ys_sem.at[kind, i], got, {'cp': to_row, 'tp': col * CORES + row // half_cp}).start()

    def share(b):
        for rr in range(half_cp):
            r = core * half_cp + rr
            some = pl.ds(0, batch_units)
            pltpu.make_async_copy(kv_all.at[r, some], kv_all.at[r, some], ykv_sem.at[rr, b]).wait()
            for o, c, h in BATCHES[b]:
                unit = unit_of(o, c, h)
                remote(kv_all.at[r, unit], kv_all.at[r, unit], ks_sem, kr_sem.at[rr, b], sibling).start()

    for b in range(len(BATCHES)):
        for o, c, h in BATCHES[b]:
            if c == 0 and o:
                direct(x_devs - o, h).wait_recv()
                handed(o, h).start()
        for o, c, h in BATCHES[b]:
            if c == 1:
                handed(o, h).wait_recv()

        @pl.loop(0, 3)
        def _(n):
            y = jnp.dot(xg[b].reshape(batch_units * half_rows, hidden), w_ref[n], preferred_element_type=f32).astype(bf16)
            for i in range(n_heads_loc):
                for u in range(batch_units):
                    stage[b, i, u, n] = y[u * half_rows:(u + 1) * half_rows, i * LANES:(i + 1) * LANES]

        exchange(b)
        if b:
            share(b - 1)
    share(len(BATCHES) - 1)

    def wo_part(t):
        return wo_all.at[pl.ds(pl.multiple_of(t * wo_rows, wo_rows), wo_rows)]

    def wo_direct(d):
        return remote(wo_ref, wo_part(tp), ws_sem.at[d - 1], wr_sem.at[x_devs - d - 1], beside(d))

    def wo_from(o):
        t = lax.rem(col + o, x_devs) * CORES + core
        return remote(wo_ref, wo_part(t), ws_sem.at[x_devs - o - 1], wr_sem.at[o - 1], beside(x_devs - o))

    def wo_handed(o):
        t = lax.rem(col + o, x_devs) * CORES + core
        return remote(wo_ref if o == 0 else wo_part(t), wo_part(t), wfs_sem.at[o], wfr_sem.at[o], sibling)

    for d in (1, 3, 2):
        wo_direct(d).start()
    wo_handed(0).start()

    for rr in range(half_cp):
        for b in range(len(BATCHES)):
            some = pl.ds(0, batch_units)
            pltpu.make_async_copy(q_all.at[rr, some], q_all.at[rr, some], yq_sem.at[rr, b]).wait()
            other = (1 - core) * half_cp + rr
            remote(kv_all.at[other, some], kv_all.at[other, some], ks_sem, kr_sem.at[rr, b], sibling).wait_recv()

    scale = LANES ** -0.5 * math.log2(math.e)
    sub_units = half_units // 2
    sub_rows = sub_units * half_rows
    repeat = half_units * half_rows // LANES
    head = col * cp_devs + row

    def scores(q, keys):
        return lax.dot_general(q, keys, (((1,), (1,)), ((), ())), preferred_element_type=f32) * scale

    def lane_sums(p):
        total = p[:, :LANES]
        for i in range(1, p.shape[1] // LANES):
            total += p[:, i * LANES:(i + 1) * LANES]
        return total

    @pl.loop(0, 2 * half_cp)
    def _(piece):
        rr, late = piece // 2, lax.rem(piece, 2)
        block = core * half_cp + rr
        place = jnp.where(late == 0, block, 2 * cp_devs - 1 - block)
        for sub in range(2):
            q = q_all[rr, pl.ds(late * half_units + sub * sub_units, sub_units)].reshape(sub_rows, LANES)
            near = (sub + 1) * sub_units
            keys = kv_all[block, pl.ds(late * half_units, near), 0].reshape(near * half_rows, LANES)
            vals = kv_all[block, pl.ds(late * half_units, near), 1].reshape(near * half_rows, LANES)
            s = scores(q, keys)
            q_at = sub * sub_rows + lax.broadcasted_iota(jnp.int32, s.shape, 0)
            s = jnp.where(lax.broadcasted_iota(jnp.int32, s.shape, 1) <= q_at, s, -1e30)
            m = jnp.broadcast_to(jnp.max(s, axis=1, keepdims=True), (sub_rows, LANES))
            p = jnp.exp2(s - jnp.concatenate([m] * (s.shape[1] // LANES), axis=1))
            m_run[...] = m
            l_run[...] = lane_sums(p)
            acc[...] = jnp.dot(p.astype(bf16), vals, preferred_element_type=f32)

            @pl.loop(0, place)
            def _(kp):
                k_block = jnp.where(kp < cp_devs, kp, 2 * cp_devs - 1 - kp)
                k_first = jnp.where(kp < cp_devs, 0, half_units)
                keys = kv_all[k_block, pl.ds(k_first, half_units), 0].reshape(half_units * half_rows, LANES)
                vals = kv_all[k_block, pl.ds(k_first, half_units), 1].reshape(half_units * half_rows, LANES)
                s = scores(q_all[rr, pl.ds(late * half_units + sub * sub_units, sub_units)].reshape(sub_rows, LANES), keys)
                before = m_run[...]
                m = jnp.maximum(before, jnp.max(s, axis=1, keepdims=True))
                p = jnp.exp2(s - jnp.concatenate([m] * repeat, axis=1))
                fade = jnp.exp2(before - m)
                m_run[...] = m
                l_run[...] = fade * l_run[...] + lane_sums(p)
                acc[...] = fade * acc[...] + jnp.dot(p.astype(bf16), vals, preferred_element_type=f32)

            o = acc[...] / jnp.sum(l_run[...], axis=1, keepdims=True)
            o_st[rr, pl.ds(late * half_units + sub * sub_units, sub_units)] = o.astype(bf16).reshape(sub_units, half_rows, LANES)

        for t in range(tp_devs // 2):
            to_tp = late * (tp_devs // 2) + t
            src = o_st.at[rr, pl.ds(to_tp * n_half, n_half)]
            own = jnp.logical_and(block == row, to_tp == tp)

            @pl.when(own)
            def _():
                pltpu.make_async_copy(src, og.at[head], or_sem).start()

            @pl.when(jnp.logical_not(own))
            def _():
                remote(src, og.at[head], os_sem, or_sem, {'cp': block, 'tp': to_tp}).start()

        @pl.when(piece == 1)
        def _():
            for o in (1, 3):
                wo_from(o).wait_recv()
                wo_handed(o).start()

    wo_from(2).wait_recv()
    wo_handed(2).start()
    pltpu.make_async_copy(og, og, or_sem).wait()
    for n in range(og.shape[0]):
        o_rows[:, n * LANES:(n + 1) * LANES] = og[n].reshape(n_half * half_rows, LANES)
    for o in range(x_devs):
        t = lax.rem(col + o, x_devs) * CORES + 1 - core
        remote(wo_part(t), wo_part(t), wfs_sem.at[o], wfr_sem.at[o], sibling).wait_recv()

    sub = hidden // LANES
    step = 2 * LANES
    rows = n_half * half_rows

    @pl.loop(0, hidden // step)
    def _(j):
        cols = pl.ds(pl.multiple_of(j * step, step), step)
        h = jnp.dot(o_rows[...], wo_all[:, cols], preferred_element_type=f32) + hid_ref[:, :, cols].reshape(rows, step).astype(f32)
        for i in range(step // LANES):
            wide[pl.ds(j * (step // LANES) + i, rows, stride=sub), :] = h[:, i * LANES:(i + 1) * LANES]

    @pl.loop(0, rows // 8)
    def _(t):
        for i in range(8):
            h_ref[t * 8 + i] = wide[pl.ds(pl.multiple_of((t * 8 + i) * sub, sub), sub), :].astype(bf16)

    for d, h in SEND_ORDER:
        direct(d, h).wait_send()
    for o in range(x_devs):
        for h in range(n_half):
            handed(o, h).wait_send()
        wo_handed(o).wait_send()
    for d in range(1, x_devs):
        wo_direct(d).wait_send()
    for i in range(n_heads_loc):
        @pl.when(core * n_heads_loc + i != row)
        def _():
            remote(q_all.at[0], q_all.at[0], ys_sem.at[0, i], yq_sem.at[0, 0], sibling).wait_send()
            remote(kv_all.at[0], kv_all.at[0], ys_sem.at[1, i], ykv_sem.at[0, 0], sibling).wait_send()
    every = kv_all.at[pl.ds(0, half_cp)]
    remote(every, every, ks_sem, kr_sem.at[0, 0], sibling).wait_send()
    own_row = row // half_cp == core

    @pl.when(own_row)
    def _():
        most = og.at[pl.ds(0, og.shape[0] - 1)]
        remote(most, most, os_sem, or_sem, sibling).wait_send()

    @pl.when(jnp.logical_not(own_row))
    def _():
        remote(og, og, os_sem, or_sem, sibling).wait_send()


def attention_residual(hidden_in, w_query, w_key, w_value, w_out, cp_devs, tp_devs):
    tok_dev, hidden = hidden_in.shape
    heads_loc, head_dim = w_query.shape[1:]
    if w_key.shape != w_query.shape or head_dim != LANES or tp_devs != RING * CORES or heads_loc * CORES != cp_devs:
        raise ValueError('unexpected sizes')
    n_half = 2
    half_rows = tok_dev // n_half
    units = tp_devs * n_half
    n_heads = heads_loc * tp_devs
    batches, batch_units = len(BATCHES), len(BATCHES[0])
    half_cp = cp_devs // 2
    sub = hidden // LANES
    sub_rows = units // 4 * half_rows
    bf16, f32 = jnp.bfloat16, jnp.float32
    dma = pltpu.SemaphoreType.DMA
    w_all = jnp.stack([w.reshape(hidden, heads_loc * head_dim) for w in (w_query, w_key, w_value)])
    return pl.pallas_call(
        functools.partial(attention_kernel, cp_devs, tp_devs),
        out_shape=jax.ShapeDtypeStruct((tok_dev, sub, LANES), bf16),
        in_specs=[pl.BlockSpec(memory_space=pltpu.VMEM)] * 3,
        out_specs=pl.BlockSpec(memory_space=pltpu.VMEM),
        scratch_shapes=[
            pltpu.VMEM((batches, batch_units, half_rows, hidden), bf16),
            pltpu.VMEM((batches, heads_loc, batch_units, 3, half_rows, LANES), bf16),
            pltpu.VMEM((half_cp, units, half_rows, LANES), bf16),
            pltpu.VMEM((cp_devs, units, 2, half_rows, LANES), bf16),
            pltpu.VMEM((half_cp, units, half_rows, LANES), bf16),
            pltpu.VMEM((n_heads, n_half, half_rows, LANES), bf16),
            pltpu.VMEM((tok_dev, hidden), bf16),
            pltpu.VMEM((n_heads * head_dim, hidden), bf16),
            pltpu.VMEM((tok_dev * sub, LANES), f32),
            pltpu.VMEM((sub_rows, LANES), f32),
            pltpu.VMEM((sub_rows, LANES), f32),
            pltpu.VMEM((sub_rows, LANES), f32),
            dma((RING - 1, n_half)), dma((RING - 1, n_half)), dma((RING, n_half)), dma((RING, n_half)),
            dma((2, heads_loc)), dma((half_cp, batches)), dma((half_cp, batches)), dma, dma((half_cp, batches)),
            dma((RING - 1,)), dma((RING - 1,)), dma((RING,)), dma((RING,)), dma, dma,
        ],
        compiler_params=pltpu.CompilerParams(collective_id=1, has_side_effects=True, vmem_limit_bytes=67043328),
        cost_estimate=pl.CostEstimate(flops=12 * 10 ** 9, bytes_accessed=16 * 10 ** 6, transcendentals=10 ** 7),
        name='attention_exchange',
    )(hidden_in.reshape(n_half, half_rows, hidden), w_all, w_out.reshape(heads_loc * head_dim, hidden))


from jax.sharding import PartitionSpec as P


def solution(mesh):
    cp_devs, tp_devs = mesh.shape['cp'], mesh.shape['tp']
    row_spec = P(('dp', 'cp', 'tp'), None)
    head_spec = P(None, 'tp', None)
    expert_spec = P(('cp', 'tp'), None, None)

    def device_step(hidden_in, w_query, w_key, w_value, w_out, expert_idx, gate_vals, w_gate, w_up, w_down):
        h_tiles = attention_residual(hidden_in, w_query, w_key, w_value, w_out, cp_devs, tp_devs)
        return moe(h_tiles, expert_idx, gate_vals, w_gate, w_up, w_down, cp_devs, tp_devs)

    return jax.shard_map(device_step, mesh=mesh, in_specs=(row_spec, head_spec, head_spec, head_spec, P('tp', None, None), row_spec, row_spec, expert_spec, expert_spec, expert_spec), out_specs=row_spec, check_vma=False)
```

```python
import functools
import math
import jax
import jax.numpy as jnp
from jax import lax
from jax.experimental import pallas as pl
from jax.experimental.pallas import tpu as pltpu

LANES = 128
VMEM_BYTES = 66 * 1024 * 1024


CORES = 2


def spread_order(cp_devs, tp_devs):
    x_devs = tp_devs // CORES
    row, col = lax.axis_index('cp'), lax.axis_index('tp') // CORES
    core = lax.rem(lax.axis_index('tp'), CORES)
    hops = lambda d, n: min(d, n - d)
    chips = [(dx, dy) for dx in range(x_devs) for dy in range(cp_devs)]
    chips.sort(key=lambda o: (-(hops(o[0], x_devs) + hops(o[1], cp_devs)), abs(hops(o[0], x_devs) - hops(o[1], cp_devs)), (o[0] * 3 + o[1] * 5) % 4))
    for dc in range(CORES):
        for dx, dy in chips:
            if dx or dy or dc:
                yield lax.rem(row + dy, cp_devs) * tp_devs + lax.rem(col + dx, x_devs) * CORES + lax.rem(core + dc, CORES)


def moe_kernel(cp_devs, tp_devs, chunks, src_ref, pos_ref, gate_ref, h_ref, wg_ref, wu_ref, wd_ref, y_ref,
               send, recv, xbuf, wgu, wdv, act, wide, zsend, ret, w_sem, loc_sem, dsend_sem, drecv_sem, rsend_sem, rrecv_sem):
    n_dev = cp_devs * tp_devs
    local_exp = wg_ref.shape[0]
    tok_dev, sub = h_ref.shape[0], h_ref.shape[1]
    slots = send.shape[2]
    rows = n_dev * slots
    gu_tiles, dn_tiles = wgu.shape[1], wdv.shape[1]
    dn_cols = wdv.shape[3]
    top_k = gate_ref.shape[0]
    back = local_exp * slots
    me = lax.axis_index('cp') * tp_devs + lax.axis_index('tp')

    def place(dev):
        return {'cp': dev // tp_devs, 'tp': lax.rem(dev, tp_devs)}

    barrier = pltpu.get_barrier_semaphore()

    def greet(p, carry):
        pl.semaphore_signal(barrier, inc=1, device_id=place(lax.rem(me + p, n_dev)), device_id_type=pl.DeviceIdType.MESH)
        return carry

    lax.fori_loop(1, n_dev, greet, 0)

    def gu_copy(e, j, half, ref):
        return pltpu.make_async_copy(ref.at[e, :, pl.ds(pl.multiple_of(j * LANES, LANES), LANES)],
                                     wgu.at[e, j, :, pl.ds(half * LANES, LANES)], w_sem.at[0, e])

    def dn_copy(e, j):
        return pltpu.make_async_copy(wd_ref.at[e, :, pl.ds(pl.multiple_of(j * dn_cols, dn_cols), dn_cols)], wdv.at[e, j], w_sem.at[1, e])

    for e in range(local_exp):
        @pl.loop(0, gu_tiles)
        def _(j):
            gu_copy(e, j, 0, wg_ref).start()
            gu_copy(e, j, 1, wu_ref).start()

        @pl.loop(0, dn_tiles)
        def _(j):
            dn_copy(e, j).start()

    def fill(dev, carry):
        for c in range(chunks):
            for s in range(slots):
                send[c, dev, s] = h_ref[src_ref[c * slots + s, dev]]
        return carry

    with jax.named_scope('m_fill'):
        lax.fori_loop(0, n_dev, fill, 0)
    with jax.named_scope('m_barrier'):
        pl.semaphore_wait(barrier, n_dev - 1)

    def dispatch(c, dev):
        return pltpu.make_async_remote_copy(src_ref=send.at[c, dev], dst_ref=recv.at[c, me], send_sem=dsend_sem.at[c], recv_sem=drecv_sem.at[c],
                                            device_id=place(dev), device_id_type=pl.DeviceIdType.MESH)

    def give_back(c, dev):
        return pltpu.make_async_remote_copy(src_ref=zsend.at[c, dev], dst_ref=ret.at[pl.ds((c * n_dev + me) * back, back)], send_sem=rsend_sem.at[c], recv_sem=rrecv_sem.at[c],
                                            device_id=place(dev), device_id_type=pl.DeviceIdType.MESH)

    def all_of(copy, c, what):
        if what == 'start':
            for dev in spread_order(cp_devs, tp_devs):
                copy(c, dev).start()
            return
        far = pl.ds(0, n_dev - 1)
        if copy is dispatch:
            every = pltpu.make_async_remote_copy(src_ref=send.at[c, far], dst_ref=recv.at[c, far], send_sem=dsend_sem.at[c], recv_sem=drecv_sem.at[c],
                                                 device_id=place(lax.rem(me + 1, n_dev)), device_id_type=pl.DeviceIdType.MESH)
        else:
            every = pltpu.make_async_remote_copy(src_ref=zsend.at[c, far], dst_ref=zsend.at[c, far], send_sem=rsend_sem.at[c], recv_sem=rrecv_sem.at[c],
                                                 device_id=place(lax.rem(me + 1, n_dev)), device_id_type=pl.DeviceIdType.MESH)
        getattr(every, what)()

    for c in range(chunks):
        with jax.named_scope('m_dstart'):
            all_of(dispatch, c, 'start')
        pltpu.make_async_copy(send.at[c, me], recv.at[c, me], loc_sem.at[c]).start()

    for c in range(chunks):
        pltpu.make_async_copy(send.at[c, me], recv.at[c, me], loc_sem.at[c]).wait()
        with jax.named_scope('m_dwait'):
            all_of(dispatch, c, 'wait_recv')

        with jax.named_scope('m_relay'):
            @pl.loop(0, n_dev)
            def _(dev):
                for s in range(slots):
                    wide[pl.ds(pl.multiple_of((dev * slots + s) * sub, sub), sub), :] = recv[c, dev, s].astype(jnp.float32)

            for q in range(sub):
                xbuf[:, q * LANES:(q + 1) * LANES] = wide[pl.ds(q, rows, stride=sub), :].astype(jnp.bfloat16)

        @pl.loop(0, local_exp)
        def _(e):
            if c == 0:
                with jax.named_scope('m_wwait'):
                    pltpu.make_async_copy(wgu.at[e], wgu.at[e], w_sem.at[0, e]).wait()
                    pltpu.make_async_copy(wdv.at[e], wdv.at[e], w_sem.at[1, e]).wait()

            with jax.named_scope('m_gu'):
                @pl.loop(0, gu_tiles)
                def _(j):
                    both = jnp.dot(xbuf[...], wgu[e, j], preferred_element_type=jnp.float32)
                    gate, up = both[:, :LANES], both[:, LANES:]
                    act[:, pl.ds(pl.multiple_of(j * LANES, LANES), LANES)] = (gate * jax.nn.sigmoid(gate) * up).astype(jnp.bfloat16)

            with jax.named_scope('m_dn'):
                @pl.loop(0, dn_tiles)
                def _(j):
                    z = jnp.dot(act[...], wdv[e, j], preferred_element_type=jnp.float32)
                    for i in range(dn_cols // LANES):
                        wide[pl.ds(j * (dn_cols // LANES) + i, rows, stride=sub), :] = z[:, i * LANES:(i + 1) * LANES]

            with jax.named_scope('m_pack'):
                @pl.loop(0, n_dev)
                def _(dev):
                    for s in range(slots):
                        zsend[c, dev, e * slots + s] = wide[pl.ds(pl.multiple_of((dev * slots + s) * sub, sub), sub), :].astype(jnp.bfloat16)

        with jax.named_scope('m_rstart'):
            all_of(give_back, c, 'start')
        pltpu.make_async_copy(zsend.at[c, me], ret.at[pl.ds((c * n_dev + me) * back, back)], loc_sem.at[chunks + c]).start()

    for c in range(chunks):
        pltpu.make_async_copy(zsend.at[c, me], ret.at[pl.ds((c * n_dev + me) * back, back)], loc_sem.at[chunks + c]).wait()
        with jax.named_scope('m_rwait'):
            all_of(give_back, c, 'wait_recv')
    for c in range(chunks):
        with jax.named_scope('m_drain'):
            all_of(dispatch, c, 'wait_send')
            all_of(give_back, c, 'wait_send')

    with jax.named_scope('m_combine'):
        group = 8

        @pl.loop(0, tok_dev // group)
        def _(g):
            for i in range(group):
                t = g * group + i
                total = gate_ref[0, t] * ret[pos_ref[0, t]].astype(jnp.float32)
                for k in range(1, top_k):
                    total += gate_ref[k, t] * ret[pos_ref[k, t]].astype(jnp.float32)
                wide[pl.ds(pl.multiple_of(t * sub, sub), sub), :] = h_ref[t].astype(jnp.float32) + total

        for q in range(sub):
            y_ref[:, q * LANES:(q + 1) * LANES] = wide[pl.ds(q, tok_dev, stride=sub), :].astype(jnp.bfloat16)


def routing_tables(expert_idx, local_exp, n_dev, chunks):
    tok_dev, top_k = expert_idx.shape
    per_dev = tok_dev * top_k // (n_dev * local_exp)
    slots = per_dev // chunks
    dev = expert_idx // local_exp
    devs = jnp.arange(n_dev)
    member = jnp.any(dev[:, :, None] == devs[None, None, :], axis=1)
    before = (jnp.arange(tok_dev)[:, None] > jnp.arange(tok_dev)[None, :]).astype(jnp.bfloat16)
    slot_all = jnp.dot(before, member.astype(jnp.bfloat16), preferred_element_type=jnp.float32).astype(jnp.int32)
    slot = jnp.sum(jnp.where(dev[:, :, None] == devs[None, None, :], slot_all[:, None, :], 0), axis=2)
    here = member[:, :, None] & (slot_all[:, :, None] == jnp.arange(per_dev)[None, None, :])
    src = jnp.sum(jnp.where(here, jnp.arange(tok_dev, dtype=jnp.int32)[:, None, None], 0), axis=0)
    pos = (((slot // slots) * n_dev + dev) * local_exp + expert_idx % local_exp) * slots + slot % slots
    return src.T, pos.T


def moe(h_tiles, expert_idx, gate_vals, w_gate, w_up, w_down, cp_devs, tp_devs, chunks=3):
    tok_dev, sub, _ = h_tiles.shape
    hidden = sub * LANES
    local_exp, _, ffn = w_gate.shape
    top_k = expert_idx.shape[1]
    n_dev = cp_devs * tp_devs
    slots = tok_dev * top_k // (n_dev * local_exp) // chunks
    rows = n_dev * slots
    gu_tiles, dn_cols = ffn // LANES, 2 * LANES
    dn_tiles = hidden // dn_cols
    src, pos = routing_tables(expert_idx, local_exp, n_dev, chunks)
    bf16, f32 = jnp.bfloat16, jnp.float32
    flops = 6 * chunks * rows * local_exp * hidden * ffn
    out = pl.pallas_call(
        functools.partial(moe_kernel, cp_devs, tp_devs, chunks),
        out_shape=jax.ShapeDtypeStruct((tok_dev, hidden), bf16),
        in_specs=[pl.BlockSpec(memory_space=pltpu.SMEM)] * 3 + [pl.BlockSpec(memory_space=pltpu.VMEM)] + [pl.BlockSpec(memory_space=pl.ANY)] * 3,
        out_specs=pl.BlockSpec(memory_space=pltpu.VMEM),
        scratch_shapes=[
            pltpu.VMEM((chunks, n_dev, slots, sub, LANES), bf16),
            pltpu.VMEM((chunks, n_dev, slots, sub, LANES), bf16),
            pltpu.VMEM((rows, hidden), bf16),
            pltpu.VMEM((local_exp, gu_tiles, hidden, 2 * LANES), bf16),
            pltpu.VMEM((local_exp, dn_tiles, ffn, dn_cols), bf16),
            pltpu.VMEM((rows, ffn), bf16),
            pltpu.VMEM((max(rows, tok_dev) * sub, LANES), f32),
            pltpu.VMEM((chunks, n_dev, local_exp * slots, sub, LANES), bf16),
            pltpu.VMEM((chunks * n_dev * local_exp * slots, sub, LANES), bf16),
            pltpu.SemaphoreType.DMA((2, local_exp)),
            pltpu.SemaphoreType.DMA((2 * chunks,)),
            pltpu.SemaphoreType.DMA((chunks,)),
            pltpu.SemaphoreType.DMA((chunks,)),
            pltpu.SemaphoreType.DMA((chunks,)),
            pltpu.SemaphoreType.DMA((chunks,)),
        ],
        compiler_params=pltpu.CompilerParams(collective_id=0, has_side_effects=True, vmem_limit_bytes=67043328),
        cost_estimate=pl.CostEstimate(flops=flops, bytes_accessed=6 * local_exp * hidden * ffn, transcendentals=rows * ffn),
        name='moe_exchange',
    )(src, pos, gate_vals.T, h_tiles, w_gate, w_up, w_down)
    return out


RING = 4
BATCHES = (((0, 0, 0), (0, 0, 1), (0, 1, 0), (0, 1, 1)),
           ((3, 0, 0), (3, 1, 0), (1, 0, 1), (1, 1, 1)),
           ((3, 0, 1), (3, 1, 1), (1, 0, 0), (1, 1, 0)),
           ((2, 0, 0), (2, 0, 1), (2, 1, 0), (2, 1, 1)))
SEND_ORDER = ((1, 0), (3, 1), (1, 1), (3, 0))
ONWARD = {(3, 0): 1, (1, 1): 3}


def attention_kernel(cp_devs, tp_devs, hid_ref, wq_ref, wk_ref, wv_ref, wo_ref, h_ref,
                     w_in, xg, stage, q_all, kv_all, o_st, og, o_rows, wo_all, wide, acc, m_run, l_run,
                     xs_sem, xr_sem, fs_sem, fr_sem, ys_sem, yq_sem, ykv_sem, ks_sem, kr_sem, ws_sem, wr_sem, wfs_sem, wfr_sem, os_sem, or_sem, in_sem):
    row, tp = lax.axis_index('cp'), lax.axis_index('tp')
    col, core = tp // CORES, lax.rem(tp, CORES)
    x_devs = tp_devs // CORES
    n_dev = cp_devs * tp_devs
    n_half, half_rows, hidden = hid_ref.shape
    units = tp_devs * n_half
    half_units = units // 2
    half_cp = cp_devs // 2
    batch_units = len(BATCHES[0])
    n_heads_loc = stage.shape[1]
    wo_rows = wo_ref.shape[0]
    f32, bf16 = jnp.float32, jnp.bfloat16
    mesh_id = pl.DeviceIdType.MESH
    sibling = {'cp': row, 'tp': col * CORES + 1 - core}

    def remote(src, dst, send_sem, recv_sem, dev):
        return pltpu.make_async_remote_copy(src_ref=src, dst_ref=dst, send_sem=send_sem, recv_sem=recv_sem, device_id=dev, device_id_type=mesh_id)

    def beside(d):
        return {'cp': row, 'tp': lax.rem(col + d, x_devs) * CORES + core}

    barrier = pltpu.get_barrier_semaphore()

    def greet(p, carry):
        dev = lax.rem(row * tp_devs + tp + p, n_dev)
        pl.semaphore_signal(barrier, inc=1, device_id={'cp': dev // tp_devs, 'tp': lax.rem(dev, tp_devs)}, device_id_type=mesh_id)
        return carry

    lax.fori_loop(1, n_dev, greet, 0)
    loads = [pltpu.make_async_copy(ref, w_in.at[n], in_sem.at[n]) for n, ref in enumerate((wq_ref, wk_ref, wv_ref))]
    loads.append(pltpu.make_async_copy(wo_ref, wo_all.at[pl.ds(pl.multiple_of(tp * wo_rows, wo_rows), wo_rows)], in_sem.at[3]))
    for load in loads:
        load.start()
    xg[0, 0] = hid_ref[0]
    xg[0, 1] = hid_ref[1]
    with jax.named_scope('a_barrier'):
        pl.semaphore_wait(barrier, n_dev - 1)

    where = {och: (b, u) for b, batch in enumerate(BATCHES) for u, och in enumerate(batch)}

    def direct(d, h):
        o = x_devs - d
        b, u = where[(o, 0, h)]
        return remote(hid_ref.at[h], xg.at[b, u], xs_sem.at[d - 1, h], xr_sem.at[o - 1, h], beside(d))

    def onward(h):
        o = 3 if h == 0 else 1
        b, u = where[(o, 0, h)]
        b2, u2 = where[(2, 0, h)]
        return remote(xg.at[b, u], xg.at[b2, u2], xs_sem.at[1, h], xr_sem.at[1, h], beside(ONWARD[(o, h)]))

    def handed(o, h):
        b, u = where[(o, 0, h)]
        b2, u2 = where[(o, 1, h)]
        src = hid_ref.at[h] if o == 0 else xg.at[b, u]
        return remote(src, xg.at[b2, u2], fs_sem.at[o, h], fr_sem.at[o, h], sibling)

    for h in range(n_half):
        handed(0, h).start()
    for d, h in SEND_ORDER:
        direct(d, h).start()

    def unit_of(o, c, h):
        return (lax.rem(col + o, x_devs) * CORES + lax.rem(core + c, CORES)) * n_half + h

    def exchange(b):
        for i in range(n_heads_loc):
            to_row = core * n_heads_loc + i
            own = to_row == row
            for u, (o, c, h) in enumerate(BATCHES[b]):
                unit = unit_of(o, c, h)
                for kind, src, dst, sem in ((0, stage.at[b, i, u, 0], q_all.at[lax.rem(row, half_cp), unit], yq_sem),
                                            (1, stage.at[b, i, u, pl.ds(1, 2)], kv_all.at[row, unit], ykv_sem)):
                    got = sem.at[lax.rem(row, half_cp), b]

                    @pl.when(own)
                    def _():
                        pltpu.make_async_copy(src, dst, got).start()

                    @pl.when(jnp.logical_not(own))
                    def _():
                        remote(src, dst, ys_sem.at[kind, i], got, {'cp': to_row, 'tp': col * CORES + row // half_cp}).start()

    def share(b):
        for rr in range(half_cp):
            r = core * half_cp + rr
            some = pl.ds(0, batch_units)
            pltpu.make_async_copy(kv_all.at[r, some], kv_all.at[r, some], ykv_sem.at[rr, b]).wait()
            for o, c, h in BATCHES[b]:
                unit = unit_of(o, c, h)
                remote(kv_all.at[r, unit], kv_all.at[r, unit], ks_sem, kr_sem.at[rr, b], sibling).start()

    part_rows = wo_rows // n_half

    def wo_part(t, h):
        return wo_all.at[pl.ds(pl.multiple_of(t * wo_rows + h * part_rows, part_rows), part_rows)]

    def column(o, other=0):
        return lax.rem(col + o, x_devs) * CORES + (1 - core if other else core)

    def wo_direct(d, h):
        return remote(wo_part(tp, h), wo_part(tp, h), ws_sem.at[d - 1, h], wr_sem.at[x_devs - d - 1, h], beside(d))

    def wo_from(o, h):
        t = column(o)
        return remote(wo_part(t, h), wo_part(t, h), ws_sem.at[o - 1, h], wr_sem.at[o - 1, h], sibling)

    def wo_onward(o, h):
        t = column(o)
        return remote(wo_part(t, h), wo_part(t, h), ws_sem.at[1, h], wr_sem.at[1, h], beside(ONWARD[(o, h)]))

    def wo_handed(o, h, other=0):
        t = column(o, other)
        return remote(wo_part(t, h), wo_part(t, h), wfs_sem.at[o, h], wfr_sem.at[o, h], sibling)

    def wo_start():
        for d, h in SEND_ORDER:
            wo_direct(d, h).start()
        for h in range(n_half):
            wo_handed(0, h).start()

    for load in loads:
        load.wait()
    for b in range(len(BATCHES)):
        with jax.named_scope('a_xwait'):
            for o, c, h in BATCHES[b]:
                if c == 0 and o:
                    (onward(h) if o == 2 else direct(x_devs - o, h)).wait_recv()
                    if (o, h) in ONWARD:
                        onward(h).start()
                    handed(o, h).start()
            for o, c, h in BATCHES[b]:
                if c == 1:
                    handed(o, h).wait_recv()

        with jax.named_scope('a_qkv'):
            @pl.loop(0, 3)
            def _(n):
                y = jnp.dot(xg[b].reshape(batch_units * half_rows, hidden), w_in[n], preferred_element_type=f32).astype(bf16)
                for i in range(n_heads_loc):
                    for u in range(batch_units):
                        stage[b, i, u, n] = y[u * half_rows:(u + 1) * half_rows, i * LANES:(i + 1) * LANES]

        with jax.named_scope('a_exch'):
            exchange(b)
            if b == len(BATCHES) - 1:
                wo_start()
        with jax.named_scope('a_share'):
            if b:
                share(b - 1)
    with jax.named_scope('a_share_last'):
        share(len(BATCHES) - 1)

    with jax.named_scope('a_kvwait'):
        for rr in range(half_cp):
            for b in range(len(BATCHES)):
                some = pl.ds(0, batch_units)
                pltpu.make_async_copy(q_all.at[rr, some], q_all.at[rr, some], yq_sem.at[rr, b]).wait()
                other = (1 - core) * half_cp + rr
                remote(kv_all.at[other, some], kv_all.at[other, some], ks_sem, kr_sem.at[rr, b], sibling).wait_recv()

    scale = LANES ** -0.5 * math.log2(math.e)
    sub_units = half_units // 2
    sub_rows = sub_units * half_rows
    repeat = half_units * half_rows // LANES
    head = col * cp_devs + row

    def scores(q, keys):
        return lax.dot_general(q, keys, (((1,), (1,)), ((), ())), preferred_element_type=f32) * scale

    def lane_sums(p):
        total = p[:, :LANES]
        for i in range(1, p.shape[1] // LANES):
            total += p[:, i * LANES:(i + 1) * LANES]
        return total

    @pl.loop(0, 2 * half_cp)
    def _(piece):
        rr, late = piece // 2, lax.rem(piece, 2)
        block = core * half_cp + rr
        place = jnp.where(late == 0, block, 2 * cp_devs - 1 - block)
        with jax.named_scope('a_flash'):
            for sub in range(2):
                q = q_all[rr, pl.ds(late * half_units + sub * sub_units, sub_units)].reshape(sub_rows, LANES)
                near = (sub + 1) * sub_units
                keys = kv_all[block, pl.ds(late * half_units, near), 0].reshape(near * half_rows, LANES)
                vals = kv_all[block, pl.ds(late * half_units, near), 1].reshape(near * half_rows, LANES)
                s = scores(q, keys)
                q_at = sub * sub_rows + lax.broadcasted_iota(jnp.int32, s.shape, 0)
                s = jnp.where(lax.broadcasted_iota(jnp.int32, s.shape, 1) <= q_at, s, -1e30)
                m = jnp.broadcast_to(jnp.max(s, axis=1, keepdims=True), (sub_rows, LANES))
                p = jnp.exp2(s - jnp.concatenate([m] * (s.shape[1] // LANES), axis=1))
                m_run[...] = m
                l_run[...] = lane_sums(p)
                acc[...] = jnp.dot(p.astype(bf16), vals, preferred_element_type=f32)

                @pl.loop(0, place)
                def _(kp):
                    k_block = jnp.where(kp < cp_devs, kp, 2 * cp_devs - 1 - kp)
                    k_first = jnp.where(kp < cp_devs, 0, half_units)
                    keys = kv_all[k_block, pl.ds(k_first, half_units), 0].reshape(half_units * half_rows, LANES)
                    vals = kv_all[k_block, pl.ds(k_first, half_units), 1].reshape(half_units * half_rows, LANES)
                    s = scores(q_all[rr, pl.ds(late * half_units + sub * sub_units, sub_units)].reshape(sub_rows, LANES), keys)
                    before = m_run[...]
                    m = jnp.maximum(before, jnp.max(s, axis=1, keepdims=True))
                    p = jnp.exp2(s - jnp.concatenate([m] * repeat, axis=1))
                    fade = jnp.exp2(before - m)
                    m_run[...] = m
                    l_run[...] = fade * l_run[...] + lane_sums(p)
                    acc[...] = fade * acc[...] + jnp.dot(p.astype(bf16), vals, preferred_element_type=f32)

                o = acc[...] / jnp.sum(l_run[...], axis=1, keepdims=True)
                o_st[rr, pl.ds(late * half_units + sub * sub_units, sub_units)] = o.astype(bf16).reshape(sub_units, half_rows, LANES)

        for t in range(tp_devs // 2):
            to_tp = late * (tp_devs // 2) + t
            src = o_st.at[rr, pl.ds(to_tp * n_half, n_half)]
            own = jnp.logical_and(block == row, to_tp == tp)

            @pl.when(own)
            def _():
                pltpu.make_async_copy(src, og.at[head], or_sem).start()

            @pl.when(jnp.logical_not(own))
            def _():
                remote(src, og.at[head], os_sem, or_sem, {'cp': block, 'tp': to_tp}).start()

        @pl.when(piece == 0)
        def _():
            for o, h in ONWARD:
                wo_from(o, h).wait_recv()
                wo_onward(o, h).start()
                wo_handed(o, h).start()

        @pl.when(piece == 2)
        def _():
            for o, h in ((3, 1), (1, 0)):
                wo_from(o, h).wait_recv()
                wo_handed(o, h).start()

    with jax.named_scope('a_wo2'):
        for h in range(n_half):
            wo_from(2, h).wait_recv()
            wo_handed(2, h).start()
    with jax.named_scope('a_owait'):
        pltpu.make_async_copy(og, og, or_sem).wait()
    for n in range(og.shape[0]):
        o_rows[:, n * LANES:(n + 1) * LANES] = og[n].reshape(n_half * half_rows, LANES)
    with jax.named_scope('a_wowait'):
        for o in range(x_devs):
            for h in range(n_half):
                wo_handed(o, h, 1).wait_recv()

    sub = hidden // LANES
    step = 2 * LANES
    rows = n_half * half_rows

    with jax.named_scope('a_proj'):
        @pl.loop(0, hidden // step)
        def _(j):
            cols = pl.ds(pl.multiple_of(j * step, step), step)
            h = jnp.dot(o_rows[...], wo_all[:, cols], preferred_element_type=f32) + hid_ref[:, :, cols].reshape(rows, step).astype(f32)
            for i in range(step // LANES):
                wide[pl.ds(j * (step // LANES) + i, rows, stride=sub), :] = h[:, i * LANES:(i + 1) * LANES]

    with jax.named_scope('a_rows'):
        @pl.loop(0, rows // 8)
        def _(t):
            for i in range(8):
                h_ref[t * 8 + i] = wide[pl.ds(pl.multiple_of((t * 8 + i) * sub, sub), sub), :].astype(bf16)

    with jax.named_scope('a_drain'):
        for d, h in SEND_ORDER:
            direct(d, h).wait_send()
        for o in range(x_devs):
            for h in range(n_half):
                handed(o, h).wait_send()
                wo_handed(o, h).wait_send()
        for d, h in SEND_ORDER:
            wo_direct(d, h).wait_send()
        for o, h in ONWARD:
            onward(h).wait_send()
            wo_onward(o, h).wait_send()
        for i in range(n_heads_loc):
            @pl.when(core * n_heads_loc + i != row)
            def _():
                remote(q_all.at[0], q_all.at[0], ys_sem.at[0, i], yq_sem.at[0, 0], sibling).wait_send()
                remote(kv_all.at[0], kv_all.at[0], ys_sem.at[1, i], ykv_sem.at[0, 0], sibling).wait_send()
        every = kv_all.at[pl.ds(0, half_cp)]
        remote(every, every, ks_sem, kr_sem.at[0, 0], sibling).wait_send()
        own_row = row // half_cp == core

        @pl.when(own_row)
        def _():
            most = og.at[pl.ds(0, og.shape[0] - 1)]
            remote(most, most, os_sem, or_sem, sibling).wait_send()

        @pl.when(jnp.logical_not(own_row))
        def _():
            remote(og, og, os_sem, or_sem, sibling).wait_send()


def attention_residual(hidden_in, w_query, w_key, w_value, w_out, cp_devs, tp_devs):
    tok_dev, hidden = hidden_in.shape
    heads_loc, head_dim = w_query.shape[1:]
    if w_key.shape != w_query.shape or head_dim != LANES or tp_devs != RING * CORES or heads_loc * CORES != cp_devs:
        raise ValueError('unexpected sizes')
    n_half = 2
    half_rows = tok_dev // n_half
    units = tp_devs * n_half
    n_heads = heads_loc * tp_devs
    batches, batch_units = len(BATCHES), len(BATCHES[0])
    half_cp = cp_devs // 2
    sub = hidden // LANES
    sub_rows = units // 4 * half_rows
    bf16, f32 = jnp.bfloat16, jnp.float32
    dma = pltpu.SemaphoreType.DMA
    flat = [w.reshape(hidden, heads_loc * head_dim) for w in (w_query, w_key, w_value)]
    return pl.pallas_call(
        functools.partial(attention_kernel, cp_devs, tp_devs),
        out_shape=jax.ShapeDtypeStruct((tok_dev, sub, LANES), bf16),
        in_specs=[pl.BlockSpec(memory_space=pltpu.VMEM)] + [pl.BlockSpec(memory_space=pl.ANY)] * 4,
        out_specs=pl.BlockSpec(memory_space=pltpu.VMEM),
        scratch_shapes=[
            pltpu.VMEM((3, hidden, heads_loc * head_dim), bf16),
            pltpu.VMEM((batches, batch_units, half_rows, hidden), bf16),
            pltpu.VMEM((batches, heads_loc, batch_units, 3, half_rows, LANES), bf16),
            pltpu.VMEM((half_cp, units, half_rows, LANES), bf16),
            pltpu.VMEM((cp_devs, units, 2, half_rows, LANES), bf16),
            pltpu.VMEM((half_cp, units, half_rows, LANES), bf16),
            pltpu.VMEM((n_heads, n_half, half_rows, LANES), bf16),
            pltpu.VMEM((tok_dev, hidden), bf16),
            pltpu.VMEM((n_heads * head_dim, hidden), bf16),
            pltpu.VMEM((tok_dev * sub, LANES), f32),
            pltpu.VMEM((sub_rows, LANES), f32),
            pltpu.VMEM((sub_rows, LANES), f32),
            pltpu.VMEM((sub_rows, LANES), f32),
            dma((RING - 1, n_half)), dma((RING - 1, n_half)), dma((RING, n_half)), dma((RING, n_half)),
            dma((2, heads_loc)), dma((half_cp, batches)), dma((half_cp, batches)), dma, dma((half_cp, batches)),
            dma((RING - 1, n_half)), dma((RING - 1, n_half)), dma((RING, n_half)), dma((RING, n_half)), dma, dma, dma((4,)),
        ],
        compiler_params=pltpu.CompilerParams(collective_id=1, has_side_effects=True, vmem_limit_bytes=67043328),
        cost_estimate=pl.CostEstimate(flops=12 * 10 ** 9, bytes_accessed=16 * 10 ** 6, transcendentals=10 ** 7),
        name='attention_exchange',
    )(hidden_in.reshape(n_half, half_rows, hidden), *flat, w_out.reshape(heads_loc * head_dim, hidden))


from jax.sharding import PartitionSpec as P


def solution(mesh):
    cp_devs, tp_devs = mesh.shape['cp'], mesh.shape['tp']
    row_spec = P(('dp', 'cp', 'tp'), None)
    head_spec = P(None, 'tp', None)
    expert_spec = P(('cp', 'tp'), None, None)

    def device_step(hidden_in, w_query, w_key, w_value, w_out, expert_idx, gate_vals, w_gate, w_up, w_down):
        h_tiles = attention_residual(hidden_in, w_query, w_key, w_value, w_out, cp_devs, tp_devs)
        return moe(h_tiles, expert_idx, gate_vals, w_gate, w_up, w_down, cp_devs, tp_devs)

    return jax.shard_map(device_step, mesh=mesh, in_specs=(row_spec, head_spec, head_spec, head_spec, P('tp', None, None), row_spec, row_spec, expert_spec, expert_spec, expert_spec), out_specs=row_spec, check_vma=False)
```

```python
import functools
import math
import jax
import jax.numpy as jnp
from jax import lax
from jax.experimental import pallas as pl
from jax.experimental.pallas import tpu as pltpu

LANES = 128
VMEM_BYTES = 66 * 1024 * 1024


CORES = 2


def spread_order(cp_devs, tp_devs):
    x_devs = tp_devs // CORES
    row, col = lax.axis_index('cp'), lax.axis_index('tp') // CORES
    core = lax.rem(lax.axis_index('tp'), CORES)
    hops = lambda d, n: min(d, n - d)
    chips = [(dx, dy) for dx in range(x_devs) for dy in range(cp_devs)]
    chips.sort(key=lambda o: (-(hops(o[0], x_devs) + hops(o[1], cp_devs)), abs(hops(o[0], x_devs) - hops(o[1], cp_devs)), (o[0] * 3 + o[1] * 5) % 4))
    for dc in range(CORES):
        for dx, dy in chips:
            if dx or dy or dc:
                yield lax.rem(row + dy, cp_devs) * tp_devs + lax.rem(col + dx, x_devs) * CORES + lax.rem(core + dc, CORES)


def moe_kernel(cp_devs, tp_devs, chunks, src_ref, pos_ref, gate_ref, h_ref, wg_ref, wu_ref, wd_ref, y_ref,
               send, recv, xbuf, wgu, wdv, act, wide, zsend, ret, w_sem, loc_sem, dsend_sem, drecv_sem, rsend_sem, rrecv_sem):
    n_dev = cp_devs * tp_devs
    local_exp = wg_ref.shape[0]
    tok_dev, sub = h_ref.shape[0], h_ref.shape[1]
    slots = send.shape[2]
    rows = n_dev * slots
    gu_tiles, dn_tiles = wgu.shape[1], wdv.shape[1]
    dn_cols = wdv.shape[3]
    top_k = gate_ref.shape[0]
    back = local_exp * slots
    me = lax.axis_index('cp') * tp_devs + lax.axis_index('tp')

    def place(dev):
        return {'cp': dev // tp_devs, 'tp': lax.rem(dev, tp_devs)}

    barrier = pltpu.get_barrier_semaphore()

    def greet(p, carry):
        pl.semaphore_signal(barrier, inc=1, device_id=place(lax.rem(me + p, n_dev)), device_id_type=pl.DeviceIdType.MESH)
        return carry

    lax.fori_loop(1, n_dev, greet, 0)

    def gu_copy(e, j, half, ref):
        return pltpu.make_async_copy(ref.at[e, :, pl.ds(pl.multiple_of(j * LANES, LANES), LANES)],
                                     wgu.at[e, j, :, pl.ds(half * LANES, LANES)], w_sem.at[0, e])

    def dn_copy(e, j):
        return pltpu.make_async_copy(wd_ref.at[e, :, pl.ds(pl.multiple_of(j * dn_cols, dn_cols), dn_cols)], wdv.at[e, j], w_sem.at[1, e])

    for e in range(local_exp):
        @pl.loop(0, gu_tiles)
        def _(j):
            gu_copy(e, j, 0, wg_ref).start()
            gu_copy(e, j, 1, wu_ref).start()

        @pl.loop(0, dn_tiles)
        def _(j):
            dn_copy(e, j).start()

    def fill(dev, carry):
        for c in range(chunks):
            for s in range(slots):
                send[c, dev, s] = h_ref[src_ref[dev, c * slots + s]]
        return carry

    with jax.named_scope('m_fill'):
        lax.fori_loop(0, n_dev, fill, 0)
    with jax.named_scope('m_barrier'):
        pl.semaphore_wait(barrier, n_dev - 1)

    def dispatch(c, dev):
        return pltpu.make_async_remote_copy(src_ref=send.at[c, dev], dst_ref=recv.at[c, me], send_sem=dsend_sem.at[c], recv_sem=drecv_sem.at[c],
                                            device_id=place(dev), device_id_type=pl.DeviceIdType.MESH)

    def give_back(c, dev):
        return pltpu.make_async_remote_copy(src_ref=zsend.at[c, dev], dst_ref=ret.at[pl.ds((c * n_dev + me) * back, back)], send_sem=rsend_sem.at[c], recv_sem=rrecv_sem.at[c],
                                            device_id=place(dev), device_id_type=pl.DeviceIdType.MESH)

    def all_of(copy, c, what):
        if what == 'start':
            for dev in spread_order(cp_devs, tp_devs):
                copy(c, dev).start()
            return
        far = pl.ds(0, n_dev - 1)
        if copy is dispatch:
            every = pltpu.make_async_remote_copy(src_ref=send.at[c, far], dst_ref=recv.at[c, far], send_sem=dsend_sem.at[c], recv_sem=drecv_sem.at[c],
                                                 device_id=place(lax.rem(me + 1, n_dev)), device_id_type=pl.DeviceIdType.MESH)
        else:
            every = pltpu.make_async_remote_copy(src_ref=zsend.at[c, far], dst_ref=zsend.at[c, far], send_sem=rsend_sem.at[c], recv_sem=rrecv_sem.at[c],
                                                 device_id=place(lax.rem(me + 1, n_dev)), device_id_type=pl.DeviceIdType.MESH)
        getattr(every, what)()

    for c in range(chunks):
        with jax.named_scope('m_dstart'):
            all_of(dispatch, c, 'start')
        pltpu.make_async_copy(send.at[c, me], recv.at[c, me], loc_sem.at[c]).start()

    for c in range(chunks):
        pltpu.make_async_copy(send.at[c, me], recv.at[c, me], loc_sem.at[c]).wait()
        with jax.named_scope('m_dwait'):
            all_of(dispatch, c, 'wait_recv')

        with jax.named_scope('m_relay'):
            @pl.loop(0, n_dev)
            def _(dev):
                for s in range(slots):
                    wide[pl.ds(pl.multiple_of((dev * slots + s) * sub, sub), sub), :] = recv[c, dev, s].astype(jnp.float32)

            for q in range(sub):
                xbuf[:, q * LANES:(q + 1) * LANES] = wide[pl.ds(q, rows, stride=sub), :].astype(jnp.bfloat16)

        @pl.loop(0, local_exp)
        def _(e):
            if c == 0:
                with jax.named_scope('m_wwait'):
                    pltpu.make_async_copy(wgu.at[e], wgu.at[e], w_sem.at[0, e]).wait()
                    pltpu.make_async_copy(wdv.at[e], wdv.at[e], w_sem.at[1, e]).wait()

            with jax.named_scope('m_gu'):
                @pl.loop(0, gu_tiles)
                def _(j):
                    both = jnp.dot(xbuf[...], wgu[e, j], preferred_element_type=jnp.float32)
                    gate, up = both[:, :LANES], both[:, LANES:]
                    act[:, pl.ds(pl.multiple_of(j * LANES, LANES), LANES)] = (gate * jax.nn.sigmoid(gate) * up).astype(jnp.bfloat16)

            with jax.named_scope('m_dn'):
                @pl.loop(0, dn_tiles)
                def _(j):
                    z = jnp.dot(act[...], wdv[e, j], preferred_element_type=jnp.float32)
                    for i in range(dn_cols // LANES):
                        wide[pl.ds(j * (dn_cols // LANES) + i, rows, stride=sub), :] = z[:, i * LANES:(i + 1) * LANES]

            with jax.named_scope('m_pack'):
                @pl.loop(0, n_dev)
                def _(dev):
                    for s in range(slots):
                        zsend[c, dev, e * slots + s] = wide[pl.ds(pl.multiple_of((dev * slots + s) * sub, sub), sub), :].astype(jnp.bfloat16)

        with jax.named_scope('m_rstart'):
            all_of(give_back, c, 'start')
        pltpu.make_async_copy(zsend.at[c, me], ret.at[pl.ds((c * n_dev + me) * back, back)], loc_sem.at[chunks + c]).start()

    for c in range(chunks):
        pltpu.make_async_copy(zsend.at[c, me], ret.at[pl.ds((c * n_dev + me) * back, back)], loc_sem.at[chunks + c]).wait()
        with jax.named_scope('m_rwait'):
            all_of(give_back, c, 'wait_recv')
    for c in range(chunks):
        with jax.named_scope('m_drain'):
            all_of(dispatch, c, 'wait_send')
            all_of(give_back, c, 'wait_send')

    with jax.named_scope('m_combine'):
        group = 8

        @pl.loop(0, tok_dev // group)
        def _(g):
            for i in range(group):
                t = g * group + i
                total = gate_ref[0, t] * ret[pos_ref[0, t]].astype(jnp.float32)
                for k in range(1, top_k):
                    total += gate_ref[k, t] * ret[pos_ref[k, t]].astype(jnp.float32)
                wide[pl.ds(pl.multiple_of(t * sub, sub), sub), :] = h_ref[t].astype(jnp.float32) + total

        for q in range(sub):
            y_ref[:, q * LANES:(q + 1) * LANES] = wide[pl.ds(q, tok_dev, stride=sub), :].astype(jnp.bfloat16)


def routing_tables(idx_ref, src_ref, pos_ref, n_dev, local_exp, chunks):
    top_k, tok_dev = idx_ref.shape
    per_dev = tok_dev * top_k // (n_dev * local_exp)
    slots = per_dev // chunks
    shape = (n_dev, tok_dev)
    devs = lax.broadcasted_iota(jnp.int32, shape, 0)
    chosen = [idx_ref[k:k + 1, :] for k in range(top_k)]
    target = [e >> (local_exp.bit_length() - 1) for e in chosen]
    member = target[0] == devs
    for d in target[1:]:
        member = jnp.logical_or(member, d == devs)
    pair = (tok_dev, tok_dev)
    before = jnp.where(lax.broadcasted_iota(jnp.int32, pair, 0) < lax.broadcasted_iota(jnp.int32, pair, 1), 1.0, 0.0).astype(jnp.bfloat16)
    slot_all = jnp.dot(jnp.where(member, 1.0, 0.0).astype(jnp.bfloat16), before, preferred_element_type=jnp.float32)
    for k in range(top_k):
        slot = jnp.sum(jnp.where(target[k] == devs, slot_all, 0.0), axis=0, keepdims=True).astype(jnp.int32)
        chunk = jnp.zeros_like(slot)
        for c in range(1, chunks):
            chunk += jnp.where(slot >= c * slots, 1, 0)
        pos_ref[k:k + 1, :] = (((chunk * n_dev + target[k]) * local_exp + chosen[k] - target[k] * local_exp) * slots) + slot - chunk * slots
    token = lax.broadcasted_iota(jnp.int32, shape, 1).astype(jnp.float32)
    lane = lax.broadcasted_iota(jnp.int32, src_ref.shape, 1)
    table = jnp.zeros(src_ref.shape, jnp.float32)
    for s in range(per_dev):
        here = jnp.sum(jnp.where(jnp.logical_and(member, slot_all == s), token, 0.0), axis=1, keepdims=True)
        table = jnp.where(lane == s, here, table)
    src_ref[...] = table.astype(jnp.int32)


def moe(h_tiles, src, pos, gate_vals, w_gate, w_up, w_down, cp_devs, tp_devs, chunks):
    tok_dev, sub, _ = h_tiles.shape
    hidden = sub * LANES
    local_exp, _, ffn = w_gate.shape
    top_k = gate_vals.shape[1]
    n_dev = cp_devs * tp_devs
    slots = tok_dev * top_k // (n_dev * local_exp) // chunks
    rows = n_dev * slots
    gu_tiles, dn_cols = ffn // LANES, 2 * LANES
    dn_tiles = hidden // dn_cols
    bf16, f32 = jnp.bfloat16, jnp.float32
    flops = 6 * chunks * rows * local_exp * hidden * ffn
    out = pl.pallas_call(
        functools.partial(moe_kernel, cp_devs, tp_devs, chunks),
        out_shape=jax.ShapeDtypeStruct((tok_dev, hidden), bf16),
        in_specs=[pl.BlockSpec(memory_space=pltpu.SMEM)] * 3 + [pl.BlockSpec(memory_space=pltpu.VMEM)] + [pl.BlockSpec(memory_space=pl.ANY)] * 3,
        out_specs=pl.BlockSpec(memory_space=pltpu.VMEM),
        scratch_shapes=[
            pltpu.VMEM((chunks, n_dev, slots, sub, LANES), bf16),
            pltpu.VMEM((chunks, n_dev, slots, sub, LANES), bf16),
            pltpu.VMEM((rows, hidden), bf16),
            pltpu.VMEM((local_exp, gu_tiles, hidden, 2 * LANES), bf16),
            pltpu.VMEM((local_exp, dn_tiles, ffn, dn_cols), bf16),
            pltpu.VMEM((rows, ffn), bf16),
            pltpu.VMEM((max(rows, tok_dev) * sub, LANES), f32),
            pltpu.VMEM((chunks, n_dev, local_exp * slots, sub, LANES), bf16),
            pltpu.VMEM((chunks * n_dev * local_exp * slots, sub, LANES), bf16),
            pltpu.SemaphoreType.DMA((2, local_exp)),
            pltpu.SemaphoreType.DMA((2 * chunks,)),
            pltpu.SemaphoreType.DMA((chunks,)),
            pltpu.SemaphoreType.DMA((chunks,)),
            pltpu.SemaphoreType.DMA((chunks,)),
            pltpu.SemaphoreType.DMA((chunks,)),
        ],
        compiler_params=pltpu.CompilerParams(collective_id=0, has_side_effects=True, vmem_limit_bytes=67043328),
        cost_estimate=pl.CostEstimate(flops=flops, bytes_accessed=6 * local_exp * hidden * ffn, transcendentals=rows * ffn),
        name='moe_exchange',
    )(src, pos, gate_vals.T, h_tiles, w_gate, w_up, w_down)
    return out


RING = 4
BATCHES = (((0, 0, 0), (0, 0, 1), (0, 1, 0), (0, 1, 1)),
           ((3, 0, 0), (3, 1, 0), (1, 0, 1), (1, 1, 1)),
           ((3, 0, 1), (3, 1, 1), (1, 0, 0), (1, 1, 0)),
           ((2, 0, 0), (2, 0, 1), (2, 1, 0), (2, 1, 1)))
STEPS = ((0, 0, 1), (1, 0, 1), (2, 0, 1), (3, 0, 2), (3, 1, 2))
SEND_ORDER = ((1, 0), (3, 1), (1, 1), (3, 0))
ONWARD = {(3, 0): 1, (1, 1): 3}


def attention_kernel(cp_devs, tp_devs, local_exp, chunks, hid_ref, wq_ref, wk_ref, wv_ref, wo_ref, idx_ref, h_ref, src_ref, pos_ref,
                     w_raw, w_in, xg, x_last, stage, stage_last, q_all, kv_all, o_st, og, o_rows, wo_all, wide, acc, m_run, l_run,
                     xs_sem, xr_sem, fs_sem, fr_sem, ons_sem, onr_sem, fls_sem, flr_sem, ys_sem, yq_sem, ykv_sem, ks_sem, kr_sem, ws_sem, wr_sem, wfs_sem, wfr_sem, wos_sem, wor_sem, vs_sem, vr_sem, us_sem, ur_sem, hs_sem, hr_sem, os_sem, or_sem, in_sem):
    row, tp = lax.axis_index('cp'), lax.axis_index('tp')
    col, core = tp // CORES, lax.rem(tp, CORES)
    x_devs = tp_devs // CORES
    n_dev = cp_devs * tp_devs
    n_half, half_rows, hidden = hid_ref.shape
    units = tp_devs * n_half
    half_units = units // 2
    half_cp = cp_devs // 2
    batch_units = len(BATCHES[0])
    n_heads_loc = stage.shape[1]
    wo_rows = wo_ref.shape[0]
    f32, bf16 = jnp.float32, jnp.bfloat16
    mesh_id = pl.DeviceIdType.MESH
    sibling = {'cp': row, 'tp': col * CORES + 1 - core}

    def remote(src, dst, send_sem, recv_sem, dev):
        return pltpu.make_async_remote_copy(src_ref=src, dst_ref=dst, send_sem=send_sem, recv_sem=recv_sem, device_id=dev, device_id_type=mesh_id)

    def beside(d):
        return {'cp': row, 'tp': lax.rem(col + d, x_devs) * CORES + core}

    barrier = pltpu.get_barrier_semaphore()

    def greet(p, carry):
        dev = lax.rem(row * tp_devs + tp + p, n_dev)
        pl.semaphore_signal(barrier, inc=1, device_id={'cp': dev // tp_devs, 'tp': lax.rem(dev, tp_devs)}, device_id_type=mesh_id)
        return carry

    lax.fori_loop(1, n_dev, greet, 0)
    loads = [pltpu.make_async_copy(ref, w_raw.at[n], in_sem.at[n]) for n, ref in enumerate((wq_ref, wk_ref, wv_ref))]
    loads.append(pltpu.make_async_copy(wo_ref, wo_all.at[pl.ds(pl.multiple_of(tp * wo_rows, wo_rows), wo_rows)], in_sem.at[3]))
    for load in loads:
        load.start()
    xg[0, 0] = hid_ref[0]
    xg[0, 1] = hid_ref[1]
    with jax.named_scope('a_barrier'):
        pl.semaphore_wait(barrier, n_dev - 1)

    where = {och: (b, u) for b, batch in enumerate(BATCHES) for u, och in enumerate(batch)}

    def direct(d, h):
        o = x_devs - d
        b, u = where[(o, 0, h)]
        return remote(hid_ref.at[h], xg.at[b, u], xs_sem.at[d - 1, h], xr_sem.at[o - 1, h], beside(d))

    last_rows = x_last.shape[2]

    def onward(h, part):
        o = 3 if h == 0 else 1
        b, u = where[(o, 0, h)]
        return remote(xg.at[b, u, pl.ds(part * last_rows, last_rows)], x_last.at[part, where[(2, 0, h)][1]], ons_sem.at[h, part], onr_sem.at[h, part],
                      beside(ONWARD[(o, h)]))

    def handed_last(h, part):
        return remote(x_last.at[part, where[(2, 0, h)][1]], x_last.at[part, where[(2, 1, h)][1]], fls_sem.at[h, part], flr_sem.at[h, part], sibling)

    def handed(o, h):
        b, u = where[(o, 0, h)]
        b2, u2 = where[(o, 1, h)]
        src = hid_ref.at[h] if o == 0 else xg.at[b, u]
        return remote(src, xg.at[b2, u2], fs_sem.at[o, h], fr_sem.at[o, h], sibling)

    for h in range(n_half):
        handed(0, h).start()
    for d, h in SEND_ORDER:
        direct(d, h).start()

    def unit_of(o, c, h):
        return (lax.rem(col + o, x_devs) * CORES + lax.rem(core + c, CORES)) * n_half + h

    def rows_of(step):
        b, part, parts = STEPS[step]
        return BATCHES[b], pl.ds(part * (half_rows // parts), half_rows // parts)

    def exchange(step):
        b, part, parts = STEPS[step]
        batch, some = rows_of(step)
        done = stage.at[b] if parts == 1 else stage_last.at[part]
        for i in range(n_heads_loc):
            to_row = core * n_heads_loc + i
            own = to_row == row
            for u, (o, c, h) in enumerate(batch):
                unit = unit_of(o, c, h)
                for kind, src, dst, sem in ((0, done.at[i, u, 0], q_all.at[lax.rem(row, half_cp), unit, some], yq_sem),
                                            (1, done.at[i, u, pl.ds(1, 2)], kv_all.at[row, unit, :, some], ykv_sem)):
                    got = sem.at[lax.rem(row, half_cp), step]

                    @pl.when(own)
                    def _():
                        pltpu.make_async_copy(src, dst, got).start()

                    @pl.when(jnp.logical_not(own))
                    def _():
                        remote(src, dst, ys_sem.at[kind, i], got, {'cp': to_row, 'tp': col * CORES + row // half_cp}).start()

    def share(step):
        batch, some = rows_of(step)
        for rr in range(half_cp):
            r = core * half_cp + rr
            every = kv_all.at[r, pl.ds(0, batch_units), :, some]
            pltpu.make_async_copy(every, every, ykv_sem.at[rr, step]).wait()
            for o, c, h in batch:
                one = kv_all.at[r, unit_of(o, c, h), :, some]
                remote(one, one, ks_sem, kr_sem.at[rr, step], sibling).start()

    ring_rows = wo_rows // (2 * n_half)
    share_rows = wo_rows // (2 * cp_devs)

    def wo_rows_at(t, first, n):
        return wo_all.at[pl.ds(pl.multiple_of(t * wo_rows + first, n), n)]

    def wo_part(t, h):
        return wo_rows_at(t, h * ring_rows, ring_rows)

    def wo_share(t):
        return wo_rows_at(t, wo_rows // 2 + row * share_rows, share_rows)

    def column(o, other=0):
        return lax.rem(col + o, x_devs) * CORES + (1 - core if other else core)

    def wo_direct(d, h):
        return remote(wo_part(tp, h), wo_part(tp, h), ws_sem.at[d - 1, h], wr_sem.at[x_devs - d - 1, h], beside(d))

    def wo_from(o, h):
        t = column(o)
        return remote(wo_part(t, h), wo_part(t, h), ws_sem.at[o - 1, h], wr_sem.at[o - 1, h], sibling)

    def wo_onward(o, h):
        t = column(o)
        return remote(wo_part(t, h), wo_part(t, h), wos_sem.at[h], wor_sem.at[h], beside(ONWARD[(o, h)]))

    def wo_handed(o, h, other=0):
        t = column(o, other)
        return remote(wo_part(t, h), wo_part(t, h), wfs_sem.at[o, h], wfr_sem.at[o, h], sibling)

    def wo_across(d):
        return remote(wo_share(tp), wo_share(tp), vs_sem.at[d - 1], vr_sem.at[x_devs - d - 1], beside(d))

    def wo_along(o, e):
        t = column(o)
        return remote(wo_share(t), wo_share(t), us_sem, ur_sem, {'cp': lax.rem(row + e, cp_devs), 'tp': tp})

    def wo_rest_handed(o, other=0):
        part = wo_rows_at(column(o, other), wo_rows // 2, wo_rows // 2)
        return remote(part, part, hs_sem.at[o], hr_sem.at[o], sibling)

    def wo_start():
        for d in range(1, x_devs):
            wo_across(d).start()
        for d, h in SEND_ORDER:
            wo_direct(d, h).start()
        for h in range(n_half):
            wo_handed(0, h).start()
        wo_rest_handed(0).start()

    def wo_spread():
        for o in range(1, x_devs):
            t = column(o)
            remote(wo_share(t), wo_share(t), vs_sem.at[o - 1], vr_sem.at[o - 1], sibling).wait_recv()
        for e in (2, 1, 3):
            for o in range(1, x_devs):
                wo_along(o, e).start()

    all_along = wo_all.at[pl.ds(0, (x_devs - 1) * (cp_devs - 1) * share_rows)]

    for load in loads:
        load.wait()
    with jax.named_scope('a_weights'):
        some_rows = 2 * LANES

        @pl.loop(0, hidden // some_rows)
        def _(i):
            at = pl.ds(pl.multiple_of(i * some_rows, some_rows), some_rows)
            for n in range(3):
                w_in[n, at, :] = w_raw[n, at].reshape(some_rows, w_in.shape[2])

    for step, (b, part, parts) in enumerate(STEPS):
        with jax.named_scope('a_xwait'):
            for o, c, h in BATCHES[b]:
                if c == 0 and o:
                    (onward(h, part) if o == 2 else direct(x_devs - o, h)).wait_recv()
                    if (o, h) in ONWARD:
                        onward(h, 0).start()
                        onward(h, 1).start()
                    (handed_last(h, part) if o == 2 else handed(o, h)).start()
            for o, c, h in BATCHES[b]:
                if c == 1:
                    (handed_last(h, part) if o == 2 else handed(o, h)).wait_recv()

        with jax.named_scope('a_qkv'):
            n_rows = half_rows // parts

            @pl.loop(0, 3)
            def _(n):
                x = xg[b] if parts == 1 else x_last[part]
                y = jnp.dot(x.reshape(batch_units * n_rows, hidden), w_in[n], preferred_element_type=f32).astype(bf16)
                for i in range(n_heads_loc):
                    for u in range(batch_units):
                        val = y[u * n_rows:(u + 1) * n_rows, i * LANES:(i + 1) * LANES]
                        if parts == 1:
                            stage[b, i, u, n] = val
                        else:
                            stage_last[part, i, u, n] = val

        with jax.named_scope('a_exch'):
            exchange(step)
            if step == 1:
                wo_start()
        with jax.named_scope('a_share'):
            if step in (1, 2):
                share(step - 1)
        if step == 0:
            with jax.named_scope('a_tables'):
                routing_tables(idx_ref, src_ref, pos_ref, n_dev, local_exp, chunks)
    with jax.named_scope('a_share_last'):
        for step in range(2, len(STEPS)):
            share(step)
    with jax.named_scope('a_wospread'):
        wo_spread()

    with jax.named_scope('a_kvwait'):
        for rr in range(half_cp):
            for step in range(len(STEPS)):
                _, some = rows_of(step)
                got = q_all.at[rr, pl.ds(0, batch_units), some]
                pltpu.make_async_copy(got, got, yq_sem.at[rr, step]).wait()
                got = kv_all.at[(1 - core) * half_cp + rr, pl.ds(0, batch_units), :, some]
                remote(got, got, ks_sem, kr_sem.at[rr, step], sibling).wait_recv()

    scale = LANES ** -0.5 * math.log2(math.e)
    sub_units = half_units // 2
    sub_rows = sub_units * half_rows
    repeat = half_units * half_rows // LANES
    head = col * cp_devs + row

    def scores(q, keys):
        return lax.dot_general(q, keys, (((1,), (1,)), ((), ())), preferred_element_type=f32) * scale

    def lane_sums(p):
        total = p[:, :LANES]
        for i in range(1, p.shape[1] // LANES):
            total += p[:, i * LANES:(i + 1) * LANES]
        return total

    @pl.loop(0, 2 * half_cp)
    def _(piece):
        rr, late = piece // 2, lax.rem(piece, 2)
        block = core * half_cp + rr
        place = jnp.where(late == 0, block, 2 * cp_devs - 1 - block)
        with jax.named_scope('a_flash'):
            def queries(sub):
                return q_all[rr, pl.ds(late * half_units + sub * sub_units, sub_units)].reshape(sub_rows, LANES)

            for sub in range(2):
                near = (sub + 1) * sub_units
                keys = kv_all[block, pl.ds(late * half_units, near), 0].reshape(near * half_rows, LANES)
                vals = kv_all[block, pl.ds(late * half_units, near), 1].reshape(near * half_rows, LANES)
                s = scores(queries(sub), keys)
                q_at = sub * sub_rows + lax.broadcasted_iota(jnp.int32, s.shape, 0)
                s = jnp.where(lax.broadcasted_iota(jnp.int32, s.shape, 1) <= q_at, s, -1e30)
                m = jnp.broadcast_to(jnp.max(s, axis=1, keepdims=True), (sub_rows, LANES))
                p = jnp.exp2(s - jnp.concatenate([m] * (s.shape[1] // LANES), axis=1))
                m_run[sub] = m
                l_run[sub] = lane_sums(p)
                acc[sub] = jnp.dot(p.astype(bf16), vals, preferred_element_type=f32)

            @pl.loop(0, place)
            def _(kp):
                k_block = jnp.where(kp < cp_devs, kp, 2 * cp_devs - 1 - kp)
                k_first = jnp.where(kp < cp_devs, 0, half_units)
                keys = kv_all[k_block, pl.ds(k_first, half_units), 0].reshape(half_units * half_rows, LANES)
                vals = kv_all[k_block, pl.ds(k_first, half_units), 1].reshape(half_units * half_rows, LANES)
                both = [scores(queries(sub), keys) for sub in range(2)]
                for sub, s in enumerate(both):
                    before = m_run[sub]
                    m = jnp.maximum(before, jnp.max(s, axis=1, keepdims=True))
                    p = jnp.exp2(s - jnp.concatenate([m] * repeat, axis=1))
                    fade = jnp.exp2(before - m)
                    m_run[sub] = m
                    l_run[sub] = fade * l_run[sub] + lane_sums(p)
                    acc[sub] = fade * acc[sub] + jnp.dot(p.astype(bf16), vals, preferred_element_type=f32)

            for sub in range(2):
                o = acc[sub] / jnp.sum(l_run[sub], axis=1, keepdims=True)
                o_st[rr, pl.ds(late * half_units + sub * sub_units, sub_units)] = o.astype(bf16).reshape(sub_units, half_rows, LANES)

        for t in range(tp_devs // 2):
            to_tp = late * (tp_devs // 2) + t
            src = o_st.at[rr, pl.ds(to_tp * n_half, n_half)]
            own = jnp.logical_and(block == row, to_tp == tp)

            @pl.when(own)
            def _():
                pltpu.make_async_copy(src, og.at[head], or_sem).start()

            @pl.when(jnp.logical_not(own))
            def _():
                remote(src, og.at[head], os_sem, or_sem, {'cp': block, 'tp': to_tp}).start()

        @pl.when(piece == 0)
        def _():
            for o, h in ONWARD:
                wo_from(o, h).wait_recv()
                wo_onward(o, h).start()
                wo_handed(o, h).start()

        @pl.when(piece == 1)
        def _():
            for o, h in ((3, 1), (1, 0)):
                wo_from(o, h).wait_recv()
                wo_handed(o, h).start()

        @pl.when(piece == 2)
        def _():
            for h in range(n_half):
                t = column(2)
                remote(wo_part(t, h), wo_part(t, h), wos_sem.at[h], wor_sem.at[h], sibling).wait_recv()
                wo_handed(2, h).start()

    remote(all_along, all_along, us_sem, ur_sem, sibling).wait_recv()
    for o in range(1, x_devs):
        wo_rest_handed(o).start()

    with jax.named_scope('a_owait'):
        pltpu.make_async_copy(og, og, or_sem).wait()
    for n in range(og.shape[0]):
        o_rows[:, n * LANES:(n + 1) * LANES] = og[n].reshape(n_half * half_rows, LANES)
    with jax.named_scope('a_wowait'):
        for o in range(x_devs):
            for h in range(n_half):
                wo_handed(o, h, 1).wait_recv()
            wo_rest_handed(o, 1).wait_recv()

    sub = hidden // LANES
    step = 2 * LANES
    rows = n_half * half_rows

    with jax.named_scope('a_proj'):
        @pl.loop(0, hidden // step)
        def _(j):
            cols = pl.ds(pl.multiple_of(j * step, step), step)
            h = jnp.dot(o_rows[...], wo_all[:, cols], preferred_element_type=f32) + hid_ref[:, :, cols].reshape(rows, step).astype(f32)
            for i in range(step // LANES):
                wide[pl.ds(j * (step // LANES) + i, rows, stride=sub), :] = h[:, i * LANES:(i + 1) * LANES]

    with jax.named_scope('a_rows'):
        @pl.loop(0, rows // 8)
        def _(t):
            for i in range(8):
                h_ref[t * 8 + i] = wide[pl.ds(pl.multiple_of((t * 8 + i) * sub, sub), sub), :].astype(bf16)

    with jax.named_scope('a_drain'):
        for d, h in SEND_ORDER:
            direct(d, h).wait_send()
        for o in range(x_devs):
            for h in range(n_half):
                if o != 2:
                    handed(o, h).wait_send()
                wo_handed(o, h).wait_send()
            wo_rest_handed(o).wait_send()
        for d, h in SEND_ORDER:
            wo_direct(d, h).wait_send()
        for d in range(1, x_devs):
            wo_across(d).wait_send()
        remote(all_along, all_along, us_sem, ur_sem, sibling).wait_send()
        for o, h in ONWARD:
            wo_onward(o, h).wait_send()
            for part in range(2):
                onward(h, part).wait_send()
                handed_last(h, part).wait_send()
        for i in range(n_heads_loc):
            @pl.when(core * n_heads_loc + i != row)
            def _():
                remote(q_all.at[0], q_all.at[0], ys_sem.at[0, i], yq_sem.at[0, 0], sibling).wait_send()
                remote(kv_all.at[0], kv_all.at[0], ys_sem.at[1, i], ykv_sem.at[0, 0], sibling).wait_send()
        every = kv_all.at[pl.ds(0, half_cp)]
        remote(every, every, ks_sem, kr_sem.at[0, 0], sibling).wait_send()
        own_row = row // half_cp == core

        @pl.when(own_row)
        def _():
            most = og.at[pl.ds(0, og.shape[0] - 1)]
            remote(most, most, os_sem, or_sem, sibling).wait_send()

        @pl.when(jnp.logical_not(own_row))
        def _():
            remote(og, og, os_sem, or_sem, sibling).wait_send()


def attention_residual(hidden_in, w_query, w_key, w_value, w_out, expert_idx, local_exp, cp_devs, tp_devs, chunks):
    tok_dev, hidden = hidden_in.shape
    heads_loc, head_dim = w_query.shape[1:]
    if w_key.shape != w_query.shape or head_dim != LANES or tp_devs != RING * CORES or heads_loc * CORES != cp_devs:
        raise ValueError('unexpected sizes')
    n_half = 2
    half_rows = tok_dev // n_half
    units = tp_devs * n_half
    n_heads = heads_loc * tp_devs
    batches, batch_units = len(BATCHES), len(BATCHES[0])
    half_cp = cp_devs // 2
    sub = hidden // LANES
    sub_rows = units // 4 * half_rows
    bf16, f32 = jnp.bfloat16, jnp.float32
    dma = pltpu.SemaphoreType.DMA
    n_dev = cp_devs * tp_devs
    return pl.pallas_call(
        functools.partial(attention_kernel, cp_devs, tp_devs, local_exp, chunks),
        out_shape=[jax.ShapeDtypeStruct((tok_dev, sub, LANES), bf16), jax.ShapeDtypeStruct((n_dev, LANES), jnp.int32),
                   jax.ShapeDtypeStruct(expert_idx.shape[::-1], jnp.int32)],
        in_specs=[pl.BlockSpec(memory_space=pltpu.VMEM)] + [pl.BlockSpec(memory_space=pl.ANY)] * 4 + [pl.BlockSpec(memory_space=pltpu.VMEM)],
        out_specs=[pl.BlockSpec(memory_space=pltpu.VMEM)] * 3,
        scratch_shapes=[
            pltpu.VMEM((3, hidden, heads_loc, head_dim), bf16),
            pltpu.VMEM((3, hidden, heads_loc * head_dim), bf16),
            pltpu.VMEM((batches - 1, batch_units, half_rows, hidden), bf16),
            pltpu.VMEM((2, batch_units, half_rows // 2, hidden), bf16),
            pltpu.VMEM((batches - 1, heads_loc, batch_units, 3, half_rows, LANES), bf16),
            pltpu.VMEM((2, heads_loc, batch_units, 3, half_rows // 2, LANES), bf16),
            pltpu.VMEM((half_cp, units, half_rows, LANES), bf16),
            pltpu.VMEM((cp_devs, units, 2, half_rows, LANES), bf16),
            pltpu.VMEM((half_cp, units, half_rows, LANES), bf16),
            pltpu.VMEM((n_heads, n_half, half_rows, LANES), bf16),
            pltpu.VMEM((tok_dev, hidden), bf16),
            pltpu.VMEM((n_heads * head_dim, hidden), bf16),
            pltpu.VMEM((tok_dev * sub, LANES), f32),
            pltpu.VMEM((2, sub_rows, LANES), f32),
            pltpu.VMEM((2, sub_rows, LANES), f32),
            pltpu.VMEM((2, sub_rows, LANES), f32),
            dma((RING - 1, n_half)), dma((RING - 1, n_half)), dma((RING, n_half)), dma((RING, n_half)),
            dma((2, 2)), dma((2, 2)), dma((2, 2)), dma((2, 2)),
            dma((2, heads_loc)), dma((half_cp, len(STEPS))), dma((half_cp, len(STEPS))), dma, dma((half_cp, len(STEPS))),
            dma((RING - 1, n_half)), dma((RING - 1, n_half)), dma((RING, n_half)), dma((RING, n_half)), dma((2,)), dma((2,)),
            dma((RING - 1,)), dma((RING - 1,)), dma, dma, dma((RING,)), dma((RING,)), dma, dma, dma((4,)),
        ],
        compiler_params=pltpu.CompilerParams(collective_id=1, has_side_effects=True, vmem_limit_bytes=67043328),
        cost_estimate=pl.CostEstimate(flops=12 * 10 ** 9, bytes_accessed=16 * 10 ** 6, transcendentals=10 ** 7),
        name='attention_exchange',
    )(hidden_in.reshape(n_half, half_rows, hidden), w_query, w_key, w_value, w_out.reshape(heads_loc * head_dim, hidden), expert_idx.T)


from jax.sharding import PartitionSpec as P


def solution(mesh):
    cp_devs, tp_devs = mesh.shape['cp'], mesh.shape['tp']
    row_spec = P(('dp', 'cp', 'tp'), None)
    head_spec = P(None, 'tp', None)
    expert_spec = P(('cp', 'tp'), None, None)

    def device_step(hidden_in, w_query, w_key, w_value, w_out, expert_idx, gate_vals, w_gate, w_up, w_down):
        chunks = 3
        h_tiles, src, pos = attention_residual(hidden_in, w_query, w_key, w_value, w_out, expert_idx, w_gate.shape[0], cp_devs, tp_devs, chunks)
        return moe(h_tiles, src, pos, gate_vals, w_gate, w_up, w_down, cp_devs, tp_devs, chunks)

    return jax.shard_map(device_step, mesh=mesh, in_specs=(row_spec, head_spec, head_spec, head_spec, P('tp', None, None), row_spec, row_spec, expert_spec, expert_spec, expert_spec), out_specs=row_spec, check_vma=False)
```

```python
import functools
import math
import jax
import jax.numpy as jnp
from jax import lax
from jax.experimental import pallas as pl
from jax.experimental.pallas import tpu as pltpu

LANES = 128
VMEM_BYTES = 66 * 1024 * 1024


CORES = 2


def spread_order(cp_devs, tp_devs):
    x_devs = tp_devs // CORES
    row, col = lax.axis_index('cp'), lax.axis_index('tp') // CORES
    core = lax.rem(lax.axis_index('tp'), CORES)
    hops = lambda d, n: min(d, n - d)
    chips = [(dx, dy) for dx in range(x_devs) for dy in range(cp_devs)]
    chips.sort(key=lambda o: (-(hops(o[0], x_devs) + hops(o[1], cp_devs)), abs(hops(o[0], x_devs) - hops(o[1], cp_devs)), (o[0] * 3 + o[1] * 5) % 4))
    for dc in range(CORES):
        for dx, dy in chips:
            if dx or dy or dc:
                yield lax.rem(row + dy, cp_devs) * tp_devs + lax.rem(col + dx, x_devs) * CORES + lax.rem(core + dc, CORES)


def moe_kernel(cp_devs, tp_devs, chunks, src_ref, pos_ref, gate_ref, h_ref, wg_ref, wu_ref, wd_ref, y_ref,
               send, recv, xbuf, wgu, wdv, act, wide, zsend, ret, w_sem, loc_sem, dsend_sem, drecv_sem, rsend_sem, rrecv_sem):
    n_dev = cp_devs * tp_devs
    local_exp = wg_ref.shape[0]
    tok_dev, sub = h_ref.shape[0], h_ref.shape[1]
    slots = send.shape[2]
    rows = n_dev * slots
    gu_tiles, dn_tiles = wgu.shape[1], wdv.shape[1]
    dn_cols = wdv.shape[3]
    top_k = gate_ref.shape[0]
    back = local_exp * slots
    me = lax.axis_index('cp') * tp_devs + lax.axis_index('tp')

    def place(dev):
        return {'cp': dev // tp_devs, 'tp': lax.rem(dev, tp_devs)}

    barrier = pltpu.get_barrier_semaphore()

    def greet(p, carry):
        pl.semaphore_signal(barrier, inc=1, device_id=place(lax.rem(me + p, n_dev)), device_id_type=pl.DeviceIdType.MESH)
        return carry

    lax.fori_loop(1, n_dev, greet, 0)

    def gu_copy(e, j, half, ref):
        return pltpu.make_async_copy(ref.at[e, :, pl.ds(pl.multiple_of(j * LANES, LANES), LANES)],
                                     wgu.at[e, j, :, pl.ds(half * LANES, LANES)], w_sem.at[0, e])

    def dn_copy(e, j):
        return pltpu.make_async_copy(wd_ref.at[e, :, pl.ds(pl.multiple_of(j * dn_cols, dn_cols), dn_cols)], wdv.at[e, j], w_sem.at[1, e])

    def fill(dev, carry):
        for c in range(chunks):
            for s in range(slots):
                send[c, dev, s] = h_ref[src_ref[dev, c * slots + s]]
        return carry

    with jax.named_scope('m_fill'):
        lax.fori_loop(0, n_dev, fill, 0)
    with jax.named_scope('m_barrier'):
        pl.semaphore_wait(barrier, n_dev - 1)

    def dispatch(c, dev):
        return pltpu.make_async_remote_copy(src_ref=send.at[c, dev], dst_ref=recv.at[c, me], send_sem=dsend_sem.at[c], recv_sem=drecv_sem.at[c],
                                            device_id=place(dev), device_id_type=pl.DeviceIdType.MESH)

    def give_back(c, dev):
        return pltpu.make_async_remote_copy(src_ref=zsend.at[c, dev], dst_ref=ret.at[pl.ds((c * n_dev + me) * back, back)], send_sem=rsend_sem.at[c], recv_sem=rrecv_sem.at[c],
                                            device_id=place(dev), device_id_type=pl.DeviceIdType.MESH)

    def all_of(copy, c, what):
        if what == 'start':
            for dev in spread_order(cp_devs, tp_devs):
                copy(c, dev).start()
            return
        far = pl.ds(0, n_dev - 1)
        if copy is dispatch:
            every = pltpu.make_async_remote_copy(src_ref=send.at[c, far], dst_ref=recv.at[c, far], send_sem=dsend_sem.at[c], recv_sem=drecv_sem.at[c],
                                                 device_id=place(lax.rem(me + 1, n_dev)), device_id_type=pl.DeviceIdType.MESH)
        else:
            every = pltpu.make_async_remote_copy(src_ref=zsend.at[c, far], dst_ref=zsend.at[c, far], send_sem=rsend_sem.at[c], recv_sem=rrecv_sem.at[c],
                                                 device_id=place(lax.rem(me + 1, n_dev)), device_id_type=pl.DeviceIdType.MESH)
        getattr(every, what)()

    for c in range(chunks):
        with jax.named_scope('m_dstart'):
            all_of(dispatch, c, 'start')
        pltpu.make_async_copy(send.at[c, me], recv.at[c, me], loc_sem.at[c]).start()

    for e in range(local_exp):
        @pl.loop(0, gu_tiles)
        def _(j):
            gu_copy(e, j, 0, wg_ref).start()
            gu_copy(e, j, 1, wu_ref).start()

        @pl.loop(0, dn_tiles)
        def _(j):
            dn_copy(e, j).start()

    for c in range(chunks):
        pltpu.make_async_copy(send.at[c, me], recv.at[c, me], loc_sem.at[c]).wait()
        with jax.named_scope('m_dwait'):
            all_of(dispatch, c, 'wait_recv')

        with jax.named_scope('m_relay'):
            @pl.loop(0, n_dev)
            def _(dev):
                for s in range(slots):
                    wide[pl.ds(pl.multiple_of((dev * slots + s) * sub, sub), sub), :] = recv[c, dev, s].astype(jnp.float32)

            for q in range(sub):
                xbuf[:, q * LANES:(q + 1) * LANES] = wide[pl.ds(q, rows, stride=sub), :].astype(jnp.bfloat16)

        @pl.loop(0, local_exp)
        def _(e):
            if c == 0:
                with jax.named_scope('m_wwait'):
                    pltpu.make_async_copy(wgu.at[e], wgu.at[e], w_sem.at[0, e]).wait()
                    pltpu.make_async_copy(wdv.at[e], wdv.at[e], w_sem.at[1, e]).wait()

            with jax.named_scope('m_gu'):
                @pl.loop(0, gu_tiles)
                def _(j):
                    both = jnp.dot(xbuf[...], wgu[e, j], preferred_element_type=jnp.float32)
                    gate, up = both[:, :LANES], both[:, LANES:]
                    act[:, pl.ds(pl.multiple_of(j * LANES, LANES), LANES)] = (gate * jax.nn.sigmoid(gate) * up).astype(jnp.bfloat16)

            with jax.named_scope('m_dn'):
                @pl.loop(0, dn_tiles)
                def _(j):
                    z = jnp.dot(act[...], wdv[e, j], preferred_element_type=jnp.float32)
                    for i in range(dn_cols // LANES):
                        wide[pl.ds(j * (dn_cols // LANES) + i, rows, stride=sub), :] = z[:, i * LANES:(i + 1) * LANES]

            with jax.named_scope('m_pack'):
                @pl.loop(0, n_dev)
                def _(dev):
                    for s in range(slots):
                        zsend[c, dev, e * slots + s] = wide[pl.ds(pl.multiple_of((dev * slots + s) * sub, sub), sub), :].astype(jnp.bfloat16)

        with jax.named_scope('m_rstart'):
            all_of(give_back, c, 'start')
        pltpu.make_async_copy(zsend.at[c, me], ret.at[pl.ds((c * n_dev + me) * back, back)], loc_sem.at[chunks + c]).start()

    for c in range(chunks):
        pltpu.make_async_copy(zsend.at[c, me], ret.at[pl.ds((c * n_dev + me) * back, back)], loc_sem.at[chunks + c]).wait()
        with jax.named_scope('m_rwait'):
            all_of(give_back, c, 'wait_recv')
    for c in range(chunks):
        with jax.named_scope('m_drain'):
            all_of(dispatch, c, 'wait_send')
            all_of(give_back, c, 'wait_send')

    with jax.named_scope('m_combine'):
        group = 8

        @pl.loop(0, tok_dev // group)
        def _(g):
            for i in range(group):
                t = g * group + i
                total = gate_ref[0, t] * ret[pos_ref[0, t]].astype(jnp.float32)
                for k in range(1, top_k):
                    total += gate_ref[k, t] * ret[pos_ref[k, t]].astype(jnp.float32)
                wide[pl.ds(pl.multiple_of(t * sub, sub), sub), :] = h_ref[t].astype(jnp.float32) + total

        for q in range(sub):
            y_ref[:, q * LANES:(q + 1) * LANES] = wide[pl.ds(q, tok_dev, stride=sub), :].astype(jnp.bfloat16)


def routing_tables(idx_ref, src_ref, pos_ref, n_dev, local_exp, chunks):
    top_k, tok_dev = idx_ref.shape
    per_dev = tok_dev * top_k // (n_dev * local_exp)
    slots = per_dev // chunks
    shape = (n_dev, tok_dev)
    devs = lax.broadcasted_iota(jnp.int32, shape, 0)
    chosen = [idx_ref[k:k + 1, :] for k in range(top_k)]
    target = [e >> (local_exp.bit_length() - 1) for e in chosen]
    member = target[0] == devs
    for d in target[1:]:
        member = jnp.logical_or(member, d == devs)
    pair = (tok_dev, tok_dev)
    before = jnp.where(lax.broadcasted_iota(jnp.int32, pair, 0) < lax.broadcasted_iota(jnp.int32, pair, 1), 1.0, 0.0).astype(jnp.bfloat16)
    slot_all = jnp.dot(jnp.where(member, 1.0, 0.0).astype(jnp.bfloat16), before, preferred_element_type=jnp.float32)
    for k in range(top_k):
        slot = jnp.sum(jnp.where(target[k] == devs, slot_all, 0.0), axis=0, keepdims=True).astype(jnp.int32)
        chunk = jnp.zeros_like(slot)
        for c in range(1, chunks):
            chunk += jnp.where(slot >= c * slots, 1, 0)
        pos_ref[k:k + 1, :] = (((chunk * n_dev + target[k]) * local_exp + chosen[k] - target[k] * local_exp) * slots) + slot - chunk * slots
    token = lax.broadcasted_iota(jnp.int32, shape, 1).astype(jnp.float32)
    lane = lax.broadcasted_iota(jnp.int32, src_ref.shape, 1)
    table = jnp.zeros(src_ref.shape, jnp.float32)
    for s in range(per_dev):
        here = jnp.sum(jnp.where(jnp.logical_and(member, slot_all == s), token, 0.0), axis=1, keepdims=True)
        table = jnp.where(lane == s, here, table)
    src_ref[...] = table.astype(jnp.int32)


def moe(h_tiles, src, pos, gate_vals, w_gate, w_up, w_down, cp_devs, tp_devs, chunks):
    tok_dev, sub, _ = h_tiles.shape
    hidden = sub * LANES
    local_exp, _, ffn = w_gate.shape
    top_k = gate_vals.shape[1]
    n_dev = cp_devs * tp_devs
    slots = tok_dev * top_k // (n_dev * local_exp) // chunks
    rows = n_dev * slots
    gu_tiles, dn_cols = ffn // LANES, 2 * LANES
    dn_tiles = hidden // dn_cols
    bf16, f32 = jnp.bfloat16, jnp.float32
    flops = 6 * chunks * rows * local_exp * hidden * ffn
    out = pl.pallas_call(
        functools.partial(moe_kernel, cp_devs, tp_devs, chunks),
        out_shape=jax.ShapeDtypeStruct((tok_dev, hidden), bf16),
        in_specs=[pl.BlockSpec(memory_space=pltpu.SMEM)] * 3 + [pl.BlockSpec(memory_space=pltpu.VMEM)] + [pl.BlockSpec(memory_space=pl.ANY)] * 3,
        out_specs=pl.BlockSpec(memory_space=pltpu.VMEM),
        scratch_shapes=[
            pltpu.VMEM((chunks, n_dev, slots, sub, LANES), bf16),
            pltpu.VMEM((chunks, n_dev, slots, sub, LANES), bf16),
            pltpu.VMEM((rows, hidden), bf16),
            pltpu.VMEM((local_exp, gu_tiles, hidden, 2 * LANES), bf16),
            pltpu.VMEM((local_exp, dn_tiles, ffn, dn_cols), bf16),
            pltpu.VMEM((rows, ffn), bf16),
            pltpu.VMEM((max(rows, tok_dev) * sub, LANES), f32),
            pltpu.VMEM((chunks, n_dev, local_exp * slots, sub, LANES), bf16),
            pltpu.VMEM((chunks * n_dev * local_exp * slots, sub, LANES), bf16),
            pltpu.SemaphoreType.DMA((2, local_exp)),
            pltpu.SemaphoreType.DMA((2 * chunks,)),
            pltpu.SemaphoreType.DMA((chunks,)),
            pltpu.SemaphoreType.DMA((chunks,)),
            pltpu.SemaphoreType.DMA((chunks,)),
            pltpu.SemaphoreType.DMA((chunks,)),
        ],
        compiler_params=pltpu.CompilerParams(collective_id=0, has_side_effects=True, vmem_limit_bytes=67043328),
        cost_estimate=pl.CostEstimate(flops=flops, bytes_accessed=6 * local_exp * hidden * ffn, transcendentals=rows * ffn),
        name='moe_exchange',
    )(src, pos, gate_vals.T, h_tiles, w_gate, w_up, w_down)
    return out


RING = 4
BATCHES = (((0, 0, 0), (0, 0, 1), (0, 1, 0), (0, 1, 1)),
           ((3, 0, 0), (3, 1, 0), (1, 0, 1), (1, 1, 1)),
           ((3, 0, 1), (3, 1, 1), (1, 0, 0), (1, 1, 0)),
           ((2, 0, 0), (2, 0, 1), (2, 1, 0), (2, 1, 1)))
STEPS = ((0, 0, 1), (1, 0, 2), (1, 1, 2), (2, 0, 2), (2, 1, 2), (3, 0, 2), (3, 1, 2))
SEND_ORDER = ((1, 0), (3, 1), (1, 1), (3, 0))
ONWARD = {(3, 0): 1, (1, 1): 3}
ORDERS = ((0, 1, 2, 3), (2, 3, 0, 1), (0, 3, 1, 2), (2, 1, 3, 0))


def pick(values, at):
    out = values[-1]
    for n in range(len(values) - 1):
        out = jnp.where(at == n, values[n], out)
    return out


def attention_kernel(cp_devs, tp_devs, local_exp, chunks, hid_ref, wq_ref, wk_ref, wv_ref, wo_ref, idx_ref, h_ref, src_ref, pos_ref,
                     w_raw, w_in, xg, x_part, stage, stage_part, q_all, kv_all, o_st, og, o_rows, wo_all, wide, acc, m_run, l_run,
                     xs_sem, xr_sem, fs_sem, fr_sem, ons_sem, onr_sem, ys_sem, yq_sem, ykv_sem, ks_sem, kr_sem, ws_sem, wr_sem, wfs_sem, wfr_sem, wos_sem, wor_sem, vs_sem, vr_sem, us_sem, ur_sem, hs_sem, hr_sem, os_sem, or_sem, in_sem):
    row, tp = lax.axis_index('cp'), lax.axis_index('tp')
    col, core = tp // CORES, lax.rem(tp, CORES)
    x_devs = tp_devs // CORES
    n_dev = cp_devs * tp_devs
    n_half, half_rows, hidden = hid_ref.shape
    units = tp_devs * n_half
    half_units = units // 2
    half_cp = cp_devs // 2
    batch_units = len(BATCHES[0])
    n_heads_loc = stage.shape[0]
    wo_rows = wo_ref.shape[0]
    f32, bf16 = jnp.float32, jnp.bfloat16
    mesh_id = pl.DeviceIdType.MESH
    sibling = {'cp': row, 'tp': col * CORES + 1 - core}

    def remote(src, dst, send_sem, recv_sem, dev):
        return pltpu.make_async_remote_copy(src_ref=src, dst_ref=dst, send_sem=send_sem, recv_sem=recv_sem, device_id=dev, device_id_type=mesh_id)

    def beside(d):
        return {'cp': row, 'tp': lax.rem(col + d, x_devs) * CORES + core}

    barrier = pltpu.get_barrier_semaphore()

    def greet(p, carry):
        dev = lax.rem(row * tp_devs + tp + p, n_dev)
        pl.semaphore_signal(barrier, inc=1, device_id={'cp': dev // tp_devs, 'tp': lax.rem(dev, tp_devs)}, device_id_type=mesh_id)
        return carry

    lax.fori_loop(1, n_dev, greet, 0)
    loads = [pltpu.make_async_copy(ref, w_raw.at[n], in_sem.at[n]) for n, ref in enumerate((wq_ref, wk_ref, wv_ref))]
    loads.append(pltpu.make_async_copy(wo_ref, wo_all.at[pl.ds(pl.multiple_of(tp * wo_rows, wo_rows), wo_rows)], in_sem.at[3]))
    for load in loads:
        load.start()
    xg[0] = hid_ref[0]
    xg[1] = hid_ref[1]
    with jax.named_scope('a_barrier'):
        pl.semaphore_wait(barrier, n_dev - 1)

    where = {och: (b, u) for b, batch in enumerate(BATCHES) for u, och in enumerate(batch)}

    part_rows = x_part.shape[3]

    def landing(o, c, h, part):
        b, u = where[(o, c, h)]
        return x_part.at[b - 1, part, u]

    def direct(d, h, part):
        o = x_devs - d
        return remote(hid_ref.at[h, pl.ds(part * part_rows, part_rows)], landing(o, 0, h, part), xs_sem.at[d - 1, h, part], xr_sem.at[o - 1, h, part], beside(d))

    def onward(h, part):
        o = 3 if h == 0 else 1
        return remote(landing(o, 0, h, part), landing(2, 0, h, part), ons_sem.at[h, part], onr_sem.at[h, part], beside(ONWARD[(o, h)]))

    def handed(o, h, part):
        return remote(landing(o, 0, h, part), landing(o, 1, h, part), fs_sem.at[o, h, part], fr_sem.at[o, h, part], sibling)

    def handed_own(h):
        return remote(hid_ref.at[h], xg.at[where[(0, 1, h)][1]], fs_sem.at[0, h, 0], fr_sem.at[0, h, 0], sibling)

    for h in range(n_half):
        handed_own(h).start()
    for d, h in SEND_ORDER:
        for part in range(2):
            direct(d, h, part).start()

    def unit_of(o, c, h):
        return (lax.rem(col + o, x_devs) * CORES + lax.rem(core + c, CORES)) * n_half + h

    def rows_of(step):
        b, part, parts = STEPS[step]
        return BATCHES[b], pl.ds(part * (half_rows // parts), half_rows // parts)

    def exchange(step):
        b, part, parts = STEPS[step]
        batch, some = rows_of(step)
        done = stage if parts == 1 else stage_part.at[b - 1, part]
        for i in range(n_heads_loc):
            to_row = core * n_heads_loc + i
            own = to_row == row
            for u, (o, c, h) in enumerate(batch):
                unit = unit_of(o, c, h)
                for kind, src, dst, sem in ((0, done.at[i, u, 0], q_all.at[lax.rem(row, half_cp), unit, some], yq_sem),
                                            (1, done.at[i, u, pl.ds(1, 2)], kv_all.at[row, unit, :, some], ykv_sem)):
                    got = sem.at[lax.rem(row, half_cp), step]

                    @pl.when(own)
                    def _():
                        pltpu.make_async_copy(src, dst, got).start()

                    @pl.when(jnp.logical_not(own))
                    def _():
                        remote(src, dst, ys_sem.at[kind, i], got, {'cp': to_row, 'tp': col * CORES + row // half_cp}).start()

    def share(step):
        batch, some = rows_of(step)
        for rr in range(half_cp):
            r = core * half_cp + rr
            every = kv_all.at[r, pl.ds(0, batch_units), :, some]
            pltpu.make_async_copy(every, every, ykv_sem.at[rr, step]).wait()
            for o, c, h in batch:
                one = kv_all.at[r, unit_of(o, c, h), :, some]
                remote(one, one, ks_sem, kr_sem.at[rr, step], sibling).start()

    ring_rows = wo_rows // (2 * n_half)
    share_rows = wo_rows // (2 * cp_devs)

    def wo_rows_at(t, first, n):
        return wo_all.at[pl.ds(pl.multiple_of(t * wo_rows + first, n), n)]

    def wo_part(t, h):
        return wo_rows_at(t, h * ring_rows, ring_rows)

    def wo_share(t):
        return wo_rows_at(t, wo_rows // 2 + row * share_rows, share_rows)

    def column(o, other=0):
        return lax.rem(col + o, x_devs) * CORES + (1 - core if other else core)

    def wo_direct(d, h):
        return remote(wo_part(tp, h), wo_part(tp, h), ws_sem.at[d - 1, h], wr_sem.at[x_devs - d - 1, h], beside(d))

    def wo_from(o, h):
        t = column(o)
        return remote(wo_part(t, h), wo_part(t, h), ws_sem.at[o - 1, h], wr_sem.at[o - 1, h], sibling)

    def wo_onward(o, h):
        t = column(o)
        return remote(wo_part(t, h), wo_part(t, h), wos_sem.at[h], wor_sem.at[h], beside(ONWARD[(o, h)]))

    def wo_handed(o, h, other=0):
        t = column(o, other)
        return remote(wo_part(t, h), wo_part(t, h), wfs_sem.at[o, h], wfr_sem.at[o, h], sibling)

    def wo_across(d):
        return remote(wo_share(tp), wo_share(tp), vs_sem.at[d - 1], vr_sem.at[x_devs - d - 1], beside(d))

    def wo_along(o, e):
        t = column(o)
        return remote(wo_share(t), wo_share(t), us_sem, ur_sem, {'cp': lax.rem(row + e, cp_devs), 'tp': tp})

    def wo_rest_handed(o, other=0):
        part = wo_rows_at(column(o, other), wo_rows // 2, wo_rows // 2)
        return remote(part, part, hs_sem.at[o], hr_sem.at[o], sibling)

    def wo_start():
        wo_across(2).start()
        for d, h in SEND_ORDER:
            wo_direct(d, h).start()
        for h in range(n_half):
            wo_handed(0, h).start()
        wo_rest_handed(0).start()

    def wo_spread():
        for o in range(1, x_devs):
            t = column(o)
            remote(wo_share(t), wo_share(t), vs_sem.at[o - 1], vr_sem.at[o - 1], sibling).wait_recv()
        for e in (2, 1, 3):
            for o in range(1, x_devs):
                wo_along(o, e).start()

    all_along = wo_all.at[pl.ds(0, (x_devs - 1) * (cp_devs - 1) * share_rows)]

    for load in loads:
        load.wait()
    with jax.named_scope('a_weights'):
        some_rows = 2 * LANES

        @pl.loop(0, hidden // some_rows)
        def _(i):
            at = pl.ds(pl.multiple_of(i * some_rows, some_rows), some_rows)
            for n in range(3):
                w_in[n, at, :] = w_raw[n, at].reshape(some_rows, w_in.shape[2])

    for step, (b, part, parts) in enumerate(STEPS):
        with jax.named_scope('a_xwait'):
            for o, c, h in BATCHES[b]:
                if c == 0 and o:
                    (onward(h, part) if o == 2 else direct(x_devs - o, h, part)).wait_recv()
                    if (o, h) in ONWARD:
                        onward(h, part).start()
                    handed(o, h, part).start()
            for o, c, h in BATCHES[b]:
                if c == 1:
                    (handed(o, h, part) if o else handed_own(h)).wait_recv()

        if step == len(STEPS) - 2:
            wo_across(1).start()
            wo_across(3).start()
        if step == len(STEPS) - 1:
            wo_start()
        with jax.named_scope('a_qkv'):
            n_rows = half_rows // parts

            @pl.loop(0, 3)
            def _(n):
                x = xg[...] if parts == 1 else x_part[b - 1, part]
                y = jnp.dot(x.reshape(batch_units * n_rows, hidden), w_in[n], preferred_element_type=f32).astype(bf16)
                for i in range(n_heads_loc):
                    for u in range(batch_units):
                        val = y[u * n_rows:(u + 1) * n_rows, i * LANES:(i + 1) * LANES]
                        if parts == 1:
                            stage[i, u, n] = val
                        else:
                            stage_part[b - 1, part, i, u, n] = val

        with jax.named_scope('a_exch'):
            exchange(step)
        with jax.named_scope('a_share'):
            if step >= 2:
                share(step - 2)
        if step == 0:
            with jax.named_scope('a_tables'):
                routing_tables(idx_ref, src_ref, pos_ref, n_dev, local_exp, chunks)
    with jax.named_scope('a_share_last'):
        for step in range(len(STEPS) - 2, len(STEPS)):
            share(step)
    with jax.named_scope('a_wospread'):
        wo_spread()

    with jax.named_scope('a_kvwait'):
        for rr in range(half_cp):
            for step in range(len(STEPS)):
                _, some = rows_of(step)
                got = q_all.at[rr, pl.ds(0, batch_units), some]
                pltpu.make_async_copy(got, got, yq_sem.at[rr, step]).wait()
                got = kv_all.at[(1 - core) * half_cp + rr, pl.ds(0, batch_units), :, some]
                remote(got, got, ks_sem, kr_sem.at[rr, step], sibling).wait_recv()

    scale = LANES ** -0.5 * math.log2(math.e)
    sub_units = half_units // 2
    sub_rows = sub_units * half_rows
    repeat = half_units * half_rows // LANES
    head = col * cp_devs + row

    def scores(q, keys):
        return lax.dot_general(q, keys, (((1,), (1,)), ((), ())), preferred_element_type=f32) * scale

    def lane_sums(p):
        total = p[:, :LANES]
        for i in range(1, p.shape[1] // LANES):
            total += p[:, i * LANES:(i + 1) * LANES]
        return total

    @pl.loop(0, 2 * half_cp)
    def _(turn):
        diagonal = lax.rem(row + col, len(ORDERS))
        piece = pick([pick([order[t] for order in ORDERS], diagonal) for t in range(len(ORDERS))], turn)
        rr, late = piece // 2, lax.rem(piece, 2)
        block = core * half_cp + rr
        place = jnp.where(late == 0, block, 2 * cp_devs - 1 - block)
        with jax.named_scope('a_flash'):
            def queries(sub):
                return q_all[rr, pl.ds(late * half_units + sub * sub_units, sub_units)].reshape(sub_rows, LANES)

            for sub in range(2):
                near = (sub + 1) * sub_units
                keys = kv_all[block, pl.ds(late * half_units, near), 0].reshape(near * half_rows, LANES)
                vals = kv_all[block, pl.ds(late * half_units, near), 1].reshape(near * half_rows, LANES)
                s = scores(queries(sub), keys)
                q_at = sub * sub_rows + lax.broadcasted_iota(jnp.int32, s.shape, 0)
                s = jnp.where(lax.broadcasted_iota(jnp.int32, s.shape, 1) <= q_at, s, -1e30)
                m = jnp.broadcast_to(jnp.max(s, axis=1, keepdims=True), (sub_rows, LANES))
                p = jnp.exp2(s - jnp.concatenate([m] * (s.shape[1] // LANES), axis=1))
                m_run[sub] = m
                l_run[sub] = lane_sums(p)
                acc[sub] = jnp.dot(p.astype(bf16), vals, preferred_element_type=f32)

            @pl.loop(0, place)
            def _(kp):
                k_block = jnp.where(kp < cp_devs, kp, 2 * cp_devs - 1 - kp)
                k_first = jnp.where(kp < cp_devs, 0, half_units)
                keys = kv_all[k_block, pl.ds(k_first, half_units), 0].reshape(half_units * half_rows, LANES)
                vals = kv_all[k_block, pl.ds(k_first, half_units), 1].reshape(half_units * half_rows, LANES)
                both = [scores(queries(sub), keys) for sub in range(2)]
                for sub, s in enumerate(both):
                    before = m_run[sub]
                    m = jnp.maximum(before, jnp.max(s, axis=1, keepdims=True))
                    p = jnp.exp2(s - jnp.concatenate([m] * repeat, axis=1))
                    fade = jnp.exp2(before - m)
                    m_run[sub] = m
                    l_run[sub] = fade * l_run[sub] + lane_sums(p)
                    acc[sub] = fade * acc[sub] + jnp.dot(p.astype(bf16), vals, preferred_element_type=f32)

            for sub in range(2):
                o = acc[sub] / jnp.sum(l_run[sub], axis=1, keepdims=True)
                o_st[rr, pl.ds(late * half_units + sub * sub_units, sub_units)] = o.astype(bf16).reshape(sub_units, half_rows, LANES)

        for t in range(tp_devs // 2):
            to_tp = late * (tp_devs // 2) + t
            src = o_st.at[rr, pl.ds(to_tp * n_half, n_half)]
            own = jnp.logical_and(block == row, to_tp == tp)

            @pl.when(own)
            def _():
                pltpu.make_async_copy(src, og.at[head], or_sem).start()

            @pl.when(jnp.logical_not(own))
            def _():
                remote(src, og.at[head], os_sem, or_sem, {'cp': block, 'tp': to_tp}).start()

        @pl.when(turn == 1)
        def _():
            for o, h in ONWARD:
                wo_from(o, h).wait_recv()
                wo_onward(o, h).start()
                wo_handed(o, h).start()

        @pl.when(turn == 2)
        def _():
            for o, h in ((3, 1), (1, 0)):
                wo_from(o, h).wait_recv()
                wo_handed(o, h).start()

    for h in range(n_half):
        t = column(2)
        remote(wo_part(t, h), wo_part(t, h), wos_sem.at[h], wor_sem.at[h], sibling).wait_recv()
        wo_handed(2, h).start()
    remote(all_along, all_along, us_sem, ur_sem, sibling).wait_recv()
    for o in range(1, x_devs):
        wo_rest_handed(o).start()

    with jax.named_scope('a_owait'):
        pltpu.make_async_copy(og, og, or_sem).wait()
    for n in range(og.shape[0]):
        o_rows[:, n * LANES:(n + 1) * LANES] = og[n].reshape(n_half * half_rows, LANES)
    with jax.named_scope('a_wowait'):
        for o in range(x_devs):
            for h in range(n_half):
                wo_handed(o, h, 1).wait_recv()
            wo_rest_handed(o, 1).wait_recv()

    sub = hidden // LANES
    step = 2 * LANES
    rows = n_half * half_rows

    with jax.named_scope('a_proj'):
        @pl.loop(0, hidden // step)
        def _(j):
            cols = pl.ds(pl.multiple_of(j * step, step), step)
            h = jnp.dot(o_rows[...], wo_all[:, cols], preferred_element_type=f32) + hid_ref[:, :, cols].reshape(rows, step).astype(f32)
            for i in range(step // LANES):
                wide[pl.ds(j * (step // LANES) + i, rows, stride=sub), :] = h[:, i * LANES:(i + 1) * LANES]

    with jax.named_scope('a_rows'):
        @pl.loop(0, rows // 8)
        def _(t):
            for i in range(8):
                h_ref[t * 8 + i] = wide[pl.ds(pl.multiple_of((t * 8 + i) * sub, sub), sub), :].astype(bf16)

    with jax.named_scope('a_drain'):
        for d, h in SEND_ORDER:
            for part in range(2):
                direct(d, h, part).wait_send()
        for o in range(x_devs):
            for h in range(n_half):
                if o:
                    for part in range(2):
                        handed(o, h, part).wait_send()
                else:
                    handed_own(h).wait_send()
                wo_handed(o, h).wait_send()
            wo_rest_handed(o).wait_send()
        for d, h in SEND_ORDER:
            wo_direct(d, h).wait_send()
        for d in range(1, x_devs):
            wo_across(d).wait_send()
        remote(all_along, all_along, us_sem, ur_sem, sibling).wait_send()
        for o, h in ONWARD:
            wo_onward(o, h).wait_send()
            for part in range(2):
                onward(h, part).wait_send()
        for i in range(n_heads_loc):
            @pl.when(core * n_heads_loc + i != row)
            def _():
                remote(q_all.at[0], q_all.at[0], ys_sem.at[0, i], yq_sem.at[0, 0], sibling).wait_send()
                remote(kv_all.at[0], kv_all.at[0], ys_sem.at[1, i], ykv_sem.at[0, 0], sibling).wait_send()
        every = kv_all.at[pl.ds(0, half_cp)]
        remote(every, every, ks_sem, kr_sem.at[0, 0], sibling).wait_send()
        own_row = row // half_cp == core

        @pl.when(own_row)
        def _():
            most = og.at[pl.ds(0, og.shape[0] - 1)]
            remote(most, most, os_sem, or_sem, sibling).wait_send()

        @pl.when(jnp.logical_not(own_row))
        def _():
            remote(og, og, os_sem, or_sem, sibling).wait_send()


def attention_residual(hidden_in, w_query, w_key, w_value, w_out, expert_idx, local_exp, cp_devs, tp_devs, chunks):
    tok_dev, hidden = hidden_in.shape
    heads_loc, head_dim = w_query.shape[1:]
    if w_key.shape != w_query.shape or head_dim != LANES or tp_devs != RING * CORES or heads_loc * CORES != cp_devs:
        raise ValueError('unexpected sizes')
    n_half = 2
    half_rows = tok_dev // n_half
    units = tp_devs * n_half
    n_heads = heads_loc * tp_devs
    batches, batch_units = len(BATCHES), len(BATCHES[0])
    half_cp = cp_devs // 2
    sub = hidden // LANES
    sub_rows = units // 4 * half_rows
    bf16, f32 = jnp.bfloat16, jnp.float32
    dma = pltpu.SemaphoreType.DMA
    n_dev = cp_devs * tp_devs
    return pl.pallas_call(
        functools.partial(attention_kernel, cp_devs, tp_devs, local_exp, chunks),
        out_shape=[jax.ShapeDtypeStruct((tok_dev, sub, LANES), bf16), jax.ShapeDtypeStruct((n_dev, LANES), jnp.int32),
                   jax.ShapeDtypeStruct(expert_idx.shape[::-1], jnp.int32)],
        in_specs=[pl.BlockSpec(memory_space=pltpu.VMEM)] + [pl.BlockSpec(memory_space=pl.ANY)] * 4 + [pl.BlockSpec(memory_space=pltpu.VMEM)],
        out_specs=[pl.BlockSpec(memory_space=pltpu.VMEM)] * 3,
        scratch_shapes=[
            pltpu.VMEM((3, hidden, heads_loc, head_dim), bf16),
            pltpu.VMEM((3, hidden, heads_loc * head_dim), bf16),
            pltpu.VMEM((batch_units, half_rows, hidden), bf16),
            pltpu.VMEM((batches - 1, 2, batch_units, half_rows // 2, hidden), bf16),
            pltpu.VMEM((heads_loc, batch_units, 3, half_rows, LANES), bf16),
            pltpu.VMEM((batches - 1, 2, heads_loc, batch_units, 3, half_rows // 2, LANES), bf16),
            pltpu.VMEM((half_cp, units, half_rows, LANES), bf16),
            pltpu.VMEM((cp_devs, units, 2, half_rows, LANES), bf16),
            pltpu.VMEM((half_cp, units, half_rows, LANES), bf16),
            pltpu.VMEM((n_heads, n_half, half_rows, LANES), bf16),
            pltpu.VMEM((tok_dev, hidden), bf16),
            pltpu.VMEM((n_heads * head_dim, hidden), bf16),
            pltpu.VMEM((tok_dev * sub, LANES), f32),
            pltpu.VMEM((2, sub_rows, LANES), f32),
            pltpu.VMEM((2, sub_rows, LANES), f32),
            pltpu.VMEM((2, sub_rows, LANES), f32),
            dma((RING - 1, n_half, 2)), dma((RING - 1, n_half, 2)), dma((RING, n_half, 2)), dma((RING, n_half, 2)),
            dma((n_half, 2)), dma((n_half, 2)),
            dma((2, heads_loc)), dma((half_cp, len(STEPS))), dma((half_cp, len(STEPS))), dma, dma((half_cp, len(STEPS))),
            dma((RING - 1, n_half)), dma((RING - 1, n_half)), dma((RING, n_half)), dma((RING, n_half)), dma((2,)), dma((2,)),
            dma((RING - 1,)), dma((RING - 1,)), dma, dma, dma((RING,)), dma((RING,)), dma, dma, dma((4,)),
        ],
        compiler_params=pltpu.CompilerParams(collective_id=1, has_side_effects=True, vmem_limit_bytes=67043328),
        cost_estimate=pl.CostEstimate(flops=12 * 10 ** 9, bytes_accessed=16 * 10 ** 6, transcendentals=10 ** 7),
        name='attention_exchange',
    )(hidden_in.reshape(n_half, half_rows, hidden), w_query, w_key, w_value, w_out.reshape(heads_loc * head_dim, hidden), expert_idx.T)


from jax.sharding import PartitionSpec as P


def solution(mesh):
    cp_devs, tp_devs = mesh.shape['cp'], mesh.shape['tp']
    row_spec = P(('dp', 'cp', 'tp'), None)
    head_spec = P(None, 'tp', None)
    expert_spec = P(('cp', 'tp'), None, None)

    def device_step(hidden_in, w_query, w_key, w_value, w_out, expert_idx, gate_vals, w_gate, w_up, w_down):
        chunks = 3
        h_tiles, src, pos = attention_residual(hidden_in, w_query, w_key, w_value, w_out, expert_idx, w_gate.shape[0], cp_devs, tp_devs, chunks)
        return moe(h_tiles, src, pos, gate_vals, w_gate, w_up, w_down, cp_devs, tp_devs, chunks)

    return jax.shard_map(device_step, mesh=mesh, in_specs=(row_spec, head_spec, head_spec, head_spec, P('tp', None, None), row_spec, row_spec, expert_spec, expert_spec, expert_spec), out_specs=row_spec, check_vma=False)
```

```python
import functools
import math
import jax
import jax.numpy as jnp
from jax import lax
from jax.experimental import pallas as pl
from jax.experimental.pallas import tpu as pltpu

LANES = 128
VMEM_BYTES = 66 * 1024 * 1024


CORES = 2


def spread_order(cp_devs, tp_devs):
    x_devs = tp_devs // CORES
    row, col = lax.axis_index('cp'), lax.axis_index('tp') // CORES
    core = lax.rem(lax.axis_index('tp'), CORES)
    hops = lambda d, n: min(d, n - d)
    chips = [(dx, dy) for dx in range(x_devs) for dy in range(cp_devs)]
    chips.sort(key=lambda o: (-(hops(o[0], x_devs) + hops(o[1], cp_devs)), abs(hops(o[0], x_devs) - hops(o[1], cp_devs)), (o[0] * 3 + o[1] * 5) % 4))
    for dc in range(CORES):
        for dx, dy in chips:
            if dx or dy or dc:
                yield lax.rem(row + dy, cp_devs) * tp_devs + lax.rem(col + dx, x_devs) * CORES + lax.rem(core + dc, CORES)


def moe_kernel(cp_devs, tp_devs, chunks, src_ref, pos_ref, gate_ref, h_ref, wg_ref, wu_ref, wd_ref, y_ref,
               send, recv, xbuf, wgu, wdv, act, wide, zsend, ret, w_sem, loc_sem, dsend_sem, drecv_sem, rsend_sem, rrecv_sem):
    n_dev = cp_devs * tp_devs
    local_exp = wg_ref.shape[0]
    tok_dev, sub = h_ref.shape[0], h_ref.shape[1]
    slots = send.shape[2]
    rows = n_dev * slots
    gu_tiles, dn_tiles = wgu.shape[1], wdv.shape[1]
    dn_cols = wdv.shape[3]
    top_k = gate_ref.shape[0]
    back = local_exp * slots
    me = lax.axis_index('cp') * tp_devs + lax.axis_index('tp')

    def place(dev):
        return {'cp': dev // tp_devs, 'tp': lax.rem(dev, tp_devs)}

    barrier = pltpu.get_barrier_semaphore()

    def greet(p, carry):
        pl.semaphore_signal(barrier, inc=1, device_id=place(lax.rem(me + p, n_dev)), device_id_type=pl.DeviceIdType.MESH)
        return carry

    lax.fori_loop(1, n_dev, greet, 0)

    def gu_copy(e, j, half, ref):
        return pltpu.make_async_copy(ref.at[e, :, pl.ds(pl.multiple_of(j * LANES, LANES), LANES)],
                                     wgu.at[e, j, :, pl.ds(half * LANES, LANES)], w_sem.at[0, e])

    def dn_copy(e, j):
        return pltpu.make_async_copy(wd_ref.at[e, :, pl.ds(pl.multiple_of(j * dn_cols, dn_cols), dn_cols)], wdv.at[e, j], w_sem.at[1, e])

    for e in range(local_exp):
        @pl.loop(0, gu_tiles)
        def _(j):
            gu_copy(e, j, 0, wg_ref).start()
            gu_copy(e, j, 1, wu_ref).start()

        @pl.loop(0, dn_tiles)
        def _(j):
            dn_copy(e, j).start()

    def fill(dev, carry):
        for c in range(chunks):
            for s in range(slots):
                send[c, dev, s] = h_ref[src_ref[dev, c * slots + s]]
        return carry

    with jax.named_scope('m_fill'):
        lax.fori_loop(0, n_dev, fill, 0)
    with jax.named_scope('m_barrier'):
        pl.semaphore_wait(barrier, n_dev - 1)

    def dispatch(c, dev):
        return pltpu.make_async_remote_copy(src_ref=send.at[c, dev], dst_ref=recv.at[c, me], send_sem=dsend_sem.at[c], recv_sem=drecv_sem.at[c],
                                            device_id=place(dev), device_id_type=pl.DeviceIdType.MESH)

    def give_back(c, dev):
        return pltpu.make_async_remote_copy(src_ref=zsend.at[c, dev], dst_ref=ret.at[pl.ds((c * n_dev + me) * back, back)], send_sem=rsend_sem.at[c], recv_sem=rrecv_sem.at[c],
                                            device_id=place(dev), device_id_type=pl.DeviceIdType.MESH)

    def all_of(copy, c, what):
        if what == 'start':
            for dev in spread_order(cp_devs, tp_devs):
                copy(c, dev).start()
            return
        far = pl.ds(0, n_dev - 1)
        if copy is dispatch:
            every = pltpu.make_async_remote_copy(src_ref=send.at[c, far], dst_ref=recv.at[c, far], send_sem=dsend_sem.at[c], recv_sem=drecv_sem.at[c],
                                                 device_id=place(lax.rem(me + 1, n_dev)), device_id_type=pl.DeviceIdType.MESH)
        else:
            every = pltpu.make_async_remote_copy(src_ref=zsend.at[c, far], dst_ref=zsend.at[c, far], send_sem=rsend_sem.at[c], recv_sem=rrecv_sem.at[c],
                                                 device_id=place(lax.rem(me + 1, n_dev)), device_id_type=pl.DeviceIdType.MESH)
        getattr(every, what)()

    for c in range(chunks):
        with jax.named_scope('m_dstart'):
            all_of(dispatch, c, 'start')
        pltpu.make_async_copy(send.at[c, me], recv.at[c, me], loc_sem.at[c]).start()

    for c in range(chunks):
        pltpu.make_async_copy(send.at[c, me], recv.at[c, me], loc_sem.at[c]).wait()
        with jax.named_scope('m_dwait'):
            all_of(dispatch, c, 'wait_recv')

        with jax.named_scope('m_relay'):
            @pl.loop(0, n_dev)
            def _(dev):
                for s in range(slots):
                    wide[pl.ds(pl.multiple_of((dev * slots + s) * sub, sub), sub), :] = recv[c, dev, s].astype(jnp.float32)

            for q in range(sub):
                xbuf[:, q * LANES:(q + 1) * LANES] = wide[pl.ds(q, rows, stride=sub), :].astype(jnp.bfloat16)

        @pl.loop(0, local_exp)
        def _(e):
            if c == 0:
                with jax.named_scope('m_wwait'):
                    pltpu.make_async_copy(wgu.at[e], wgu.at[e], w_sem.at[0, e]).wait()
                    pltpu.make_async_copy(wdv.at[e], wdv.at[e], w_sem.at[1, e]).wait()

            with jax.named_scope('m_gu'):
                @pl.loop(0, gu_tiles)
                def _(j):
                    both = jnp.dot(xbuf[...], wgu[e, j], preferred_element_type=jnp.float32)
                    gate, up = both[:, :LANES], both[:, LANES:]
                    act[:, pl.ds(pl.multiple_of(j * LANES, LANES), LANES)] = (gate * jax.nn.sigmoid(gate) * up).astype(jnp.bfloat16)

            with jax.named_scope('m_dn'):
                @pl.loop(0, dn_tiles)
                def _(j):
                    z = jnp.dot(act[...], wdv[e, j], preferred_element_type=jnp.float32)
                    for i in range(dn_cols // LANES):
                        wide[pl.ds(j * (dn_cols // LANES) + i, rows, stride=sub), :] = z[:, i * LANES:(i + 1) * LANES]

            with jax.named_scope('m_pack'):
                @pl.loop(0, n_dev)
                def _(dev):
                    for s in range(slots):
                        zsend[c, dev, e * slots + s] = wide[pl.ds(pl.multiple_of((dev * slots + s) * sub, sub), sub), :].astype(jnp.bfloat16)

        with jax.named_scope('m_rstart'):
            all_of(give_back, c, 'start')
        pltpu.make_async_copy(zsend.at[c, me], ret.at[pl.ds((c * n_dev + me) * back, back)], loc_sem.at[chunks + c]).start()

    for c in range(chunks):
        pltpu.make_async_copy(zsend.at[c, me], ret.at[pl.ds((c * n_dev + me) * back, back)], loc_sem.at[chunks + c]).wait()
        with jax.named_scope('m_rwait'):
            all_of(give_back, c, 'wait_recv')
    for c in range(chunks):
        with jax.named_scope('m_drain'):
            all_of(dispatch, c, 'wait_send')
            all_of(give_back, c, 'wait_send')

    with jax.named_scope('m_combine'):
        group = 8

        @pl.loop(0, tok_dev // group)
        def _(g):
            for i in range(group):
                t = g * group + i
                total = gate_ref[0, t] * ret[pos_ref[0, t]].astype(jnp.float32)
                for k in range(1, top_k):
                    total += gate_ref[k, t] * ret[pos_ref[k, t]].astype(jnp.float32)
                wide[pl.ds(pl.multiple_of(t * sub, sub), sub), :] = h_ref[t].astype(jnp.float32) + total

        for q in range(sub):
            y_ref[:, q * LANES:(q + 1) * LANES] = wide[pl.ds(q, tok_dev, stride=sub), :].astype(jnp.bfloat16)


def routing_tables(idx_ref, src_ref, pos_ref, n_dev, local_exp, chunks):
    top_k, tok_dev = idx_ref.shape
    per_dev = tok_dev * top_k // (n_dev * local_exp)
    slots = per_dev // chunks
    shape = (n_dev, tok_dev)
    devs = lax.broadcasted_iota(jnp.int32, shape, 0)
    chosen = [idx_ref[k:k + 1, :] for k in range(top_k)]
    target = [e >> (local_exp.bit_length() - 1) for e in chosen]
    member = target[0] == devs
    for d in target[1:]:
        member = jnp.logical_or(member, d == devs)
    pair = (tok_dev, tok_dev)
    before = jnp.where(lax.broadcasted_iota(jnp.int32, pair, 0) < lax.broadcasted_iota(jnp.int32, pair, 1), 1.0, 0.0).astype(jnp.bfloat16)
    slot_all = jnp.dot(jnp.where(member, 1.0, 0.0).astype(jnp.bfloat16), before, preferred_element_type=jnp.float32)
    for k in range(top_k):
        slot = jnp.sum(jnp.where(target[k] == devs, slot_all, 0.0), axis=0, keepdims=True).astype(jnp.int32)
        chunk = jnp.zeros_like(slot)
        for c in range(1, chunks):
            chunk += jnp.where(slot >= c * slots, 1, 0)
        pos_ref[k:k + 1, :] = (((chunk * n_dev + target[k]) * local_exp + chosen[k] - target[k] * local_exp) * slots) + slot - chunk * slots
    token = lax.broadcasted_iota(jnp.int32, shape, 1).astype(jnp.float32)
    lane = lax.broadcasted_iota(jnp.int32, src_ref.shape, 1)
    table = jnp.zeros(src_ref.shape, jnp.float32)
    for s in range(per_dev):
        here = jnp.sum(jnp.where(jnp.logical_and(member, slot_all == s), token, 0.0), axis=1, keepdims=True)
        table = jnp.where(lane == s, here, table)
    src_ref[...] = table.astype(jnp.int32)


def moe(h_tiles, src, pos, gate_vals, w_gate, w_up, w_down, cp_devs, tp_devs, chunks):
    tok_dev, sub, _ = h_tiles.shape
    hidden = sub * LANES
    local_exp, _, ffn = w_gate.shape
    top_k = gate_vals.shape[1]
    n_dev = cp_devs * tp_devs
    slots = tok_dev * top_k // (n_dev * local_exp) // chunks
    rows = n_dev * slots
    gu_tiles, dn_cols = ffn // LANES, 2 * LANES
    dn_tiles = hidden // dn_cols
    bf16, f32 = jnp.bfloat16, jnp.float32
    flops = 6 * chunks * rows * local_exp * hidden * ffn
    out = pl.pallas_call(
        functools.partial(moe_kernel, cp_devs, tp_devs, chunks),
        out_shape=jax.ShapeDtypeStruct((tok_dev, hidden), bf16),
        in_specs=[pl.BlockSpec(memory_space=pltpu.SMEM)] * 3 + [pl.BlockSpec(memory_space=pltpu.VMEM)] + [pl.BlockSpec(memory_space=pl.ANY)] * 3,
        out_specs=pl.BlockSpec(memory_space=pltpu.VMEM),
        scratch_shapes=[
            pltpu.VMEM((chunks, n_dev, slots, sub, LANES), bf16),
            pltpu.VMEM((chunks, n_dev, slots, sub, LANES), bf16),
            pltpu.VMEM((rows, hidden), bf16),
            pltpu.VMEM((local_exp, gu_tiles, hidden, 2 * LANES), bf16),
            pltpu.VMEM((local_exp, dn_tiles, ffn, dn_cols), bf16),
            pltpu.VMEM((rows, ffn), bf16),
            pltpu.VMEM((max(rows, tok_dev) * sub, LANES), f32),
            pltpu.VMEM((chunks, n_dev, local_exp * slots, sub, LANES), bf16),
            pltpu.VMEM((chunks * n_dev * local_exp * slots, sub, LANES), bf16),
            pltpu.SemaphoreType.DMA((2, local_exp)),
            pltpu.SemaphoreType.DMA((2 * chunks,)),
            pltpu.SemaphoreType.DMA((chunks,)),
            pltpu.SemaphoreType.DMA((chunks,)),
            pltpu.SemaphoreType.DMA((chunks,)),
            pltpu.SemaphoreType.DMA((chunks,)),
        ],
        compiler_params=pltpu.CompilerParams(collective_id=0, has_side_effects=True, vmem_limit_bytes=67043328),
        cost_estimate=pl.CostEstimate(flops=flops, bytes_accessed=6 * local_exp * hidden * ffn, transcendentals=rows * ffn),
        name='moe_exchange',
    )(src, pos, gate_vals.T, h_tiles, w_gate, w_up, w_down)
    return out


RING = 4
BATCHES = (((0, 0, 0), (0, 0, 1), (0, 1, 0), (0, 1, 1)),
           ((3, 0, 0), (3, 1, 0), (1, 0, 1), (1, 1, 1)),
           ((3, 0, 1), (3, 1, 1), (1, 0, 0), (1, 1, 0)),
           ((2, 0, 0), (2, 0, 1), (2, 1, 0), (2, 1, 1)))
STEPS = ((0, 0, 1), (1, 0, 2), (1, 1, 2), (2, 0, 2), (2, 1, 2), (3, 0, 2), (3, 1, 2))
SEND_ORDER = ((1, 0), (3, 1), (1, 1), (3, 0))
ONWARD = {(3, 0): 1, (1, 1): 3}
ORDERS = ((0, 1, 2, 3), (2, 3, 0, 1), (0, 3, 1, 2), (2, 1, 3, 0))


def pick(values, at):
    out = values[-1]
    for n in range(len(values) - 1):
        out = jnp.where(at == n, values[n], out)
    return out


def attention_kernel(cp_devs, tp_devs, local_exp, chunks, hid_ref, wq_ref, wk_ref, wv_ref, wo_ref, idx_ref, h_ref, src_ref, pos_ref,
                     w_raw, w_in, xg, x_part, stage, stage_part, q_all, kv_all, o_st, og, o_rows, wo_all, wide, acc, m_run, l_run,
                     xs_sem, xr_sem, fs_sem, fr_sem, ons_sem, onr_sem, ys_sem, yq_sem, ykv_sem, ks_sem, kr_sem, ws_sem, wr_sem, wfs_sem, wfr_sem, wos_sem, wor_sem, vs_sem, vr_sem, us_sem, ur_sem, hs_sem, hr_sem, os_sem, or_sem, in_sem):
    row, tp = lax.axis_index('cp'), lax.axis_index('tp')
    col, core = tp // CORES, lax.rem(tp, CORES)
    x_devs = tp_devs // CORES
    n_dev = cp_devs * tp_devs
    n_half, half_rows, hidden = hid_ref.shape
    units = tp_devs * n_half
    half_units = units // 2
    half_cp = cp_devs // 2
    batch_units = len(BATCHES[0])
    n_heads_loc = stage.shape[0]
    wo_rows = wo_ref.shape[0]
    f32, bf16 = jnp.float32, jnp.bfloat16
    mesh_id = pl.DeviceIdType.MESH
    sibling = {'cp': row, 'tp': col * CORES + 1 - core}

    def remote(src, dst, send_sem, recv_sem, dev):
        return pltpu.make_async_remote_copy(src_ref=src, dst_ref=dst, send_sem=send_sem, recv_sem=recv_sem, device_id=dev, device_id_type=mesh_id)

    def beside(d):
        return {'cp': row, 'tp': lax.rem(col + d, x_devs) * CORES + core}

    barrier = pltpu.get_barrier_semaphore()

    def greet(p, carry):
        dev = lax.rem(row * tp_devs + tp + p, n_dev)
        pl.semaphore_signal(barrier, inc=1, device_id={'cp': dev // tp_devs, 'tp': lax.rem(dev, tp_devs)}, device_id_type=mesh_id)
        return carry

    lax.fori_loop(1, n_dev, greet, 0)
    loads = [pltpu.make_async_copy(ref, w_raw.at[n], in_sem.at[n]) for n, ref in enumerate((wq_ref, wk_ref, wv_ref))]
    loads.append(pltpu.make_async_copy(wo_ref, wo_all.at[pl.ds(pl.multiple_of(tp * wo_rows, wo_rows), wo_rows)], in_sem.at[3]))
    for load in loads:
        load.start()
    xg[0] = hid_ref[0]
    xg[1] = hid_ref[1]
    with jax.named_scope('a_barrier'):
        pl.semaphore_wait(barrier, n_dev - 1)

    where = {och: (b, u) for b, batch in enumerate(BATCHES) for u, och in enumerate(batch)}

    part_rows = x_part.shape[3]

    def landing(o, c, h, part):
        b, u = where[(o, c, h)]
        return x_part.at[b - 1, part, u]

    def direct(d, h, part):
        o = x_devs - d
        return remote(hid_ref.at[h, pl.ds(part * part_rows, part_rows)], landing(o, 0, h, part), xs_sem.at[d - 1, h, part], xr_sem.at[o - 1, h, part], beside(d))

    def onward(h, part):
        o = 3 if h == 0 else 1
        return remote(landing(o, 0, h, part), landing(2, 0, h, part), ons_sem.at[h, part], onr_sem.at[h, part], beside(ONWARD[(o, h)]))

    def handed(o, h, part):
        return remote(landing(o, 0, h, part), landing(o, 1, h, part), fs_sem.at[o, h, part], fr_sem.at[o, h, part], sibling)

    def handed_own(h):
        return remote(hid_ref.at[h], xg.at[where[(0, 1, h)][1]], fs_sem.at[0, h, 0], fr_sem.at[0, h, 0], sibling)

    for h in range(n_half):
        handed_own(h).start()
    for d, h in SEND_ORDER:
        for part in range(2):
            direct(d, h, part).start()

    def unit_of(o, c, h):
        return (lax.rem(col + o, x_devs) * CORES + lax.rem(core + c, CORES)) * n_half + h

    def rows_of(step):
        b, part, parts = STEPS[step]
        return BATCHES[b], pl.ds(part * (half_rows // parts), half_rows // parts)

    def exchange(step):
        b, part, parts = STEPS[step]
        batch, some = rows_of(step)
        done = stage if parts == 1 else stage_part.at[b - 1, part]
        for i in range(n_heads_loc):
            to_row = core * n_heads_loc + i
            own = to_row == row
            for u, (o, c, h) in enumerate(batch):
                unit = unit_of(o, c, h)
                for kind, src, dst, sem in ((0, done.at[i, u, 0], q_all.at[lax.rem(row, half_cp), unit, some], yq_sem),
                                            (1, done.at[i, u, pl.ds(1, 2)], kv_all.at[row, unit, :, some], ykv_sem)):
                    got = sem.at[lax.rem(row, half_cp), step]

                    @pl.when(own)
                    def _():
                        pltpu.make_async_copy(src, dst, got).start()

                    @pl.when(jnp.logical_not(own))
                    def _():
                        remote(src, dst, ys_sem.at[kind, i], got, {'cp': to_row, 'tp': col * CORES + row // half_cp}).start()

    def share(step):
        batch, some = rows_of(step)
        for rr in range(half_cp):
            r = core * half_cp + rr
            every = kv_all.at[r, pl.ds(0, batch_units), :, some]
            pltpu.make_async_copy(every, every, ykv_sem.at[rr, step]).wait()
            for o, c, h in batch:
                one = kv_all.at[r, unit_of(o, c, h), :, some]
                remote(one, one, ks_sem, kr_sem.at[rr, step], sibling).start()

    ring_rows = wo_rows // (2 * n_half)
    share_rows = wo_rows // (2 * cp_devs)

    def wo_rows_at(t, first, n):
        return wo_all.at[pl.ds(pl.multiple_of(t * wo_rows + first, n), n)]

    def wo_part(t, h):
        return wo_rows_at(t, h * ring_rows, ring_rows)

    def wo_share(t):
        return wo_rows_at(t, wo_rows // 2 + row * share_rows, share_rows)

    def column(o, other=0):
        return lax.rem(col + o, x_devs) * CORES + (1 - core if other else core)

    def wo_direct(d, h):
        return remote(wo_part(tp, h), wo_part(tp, h), ws_sem.at[d - 1, h], wr_sem.at[x_devs - d - 1, h], beside(d))

    def wo_from(o, h):
        t = column(o)
        return remote(wo_part(t, h), wo_part(t, h), ws_sem.at[o - 1, h], wr_sem.at[o - 1, h], sibling)

    def wo_onward(o, h):
        t = column(o)
        return remote(wo_part(t, h), wo_part(t, h), wos_sem.at[h], wor_sem.at[h], beside(ONWARD[(o, h)]))

    def wo_handed(o, h, other=0):
        t = column(o, other)
        return remote(wo_part(t, h), wo_part(t, h), wfs_sem.at[o, h], wfr_sem.at[o, h], sibling)

    def wo_across(d):
        return remote(wo_share(tp), wo_share(tp), vs_sem.at[d - 1], vr_sem.at[x_devs - d - 1], beside(d))

    def wo_along(o, e):
        t = column(o)
        return remote(wo_share(t), wo_share(t), us_sem, ur_sem, {'cp': lax.rem(row + e, cp_devs), 'tp': tp})

    def wo_rest_handed(o, other=0):
        part = wo_rows_at(column(o, other), wo_rows // 2, wo_rows // 2)
        return remote(part, part, hs_sem.at[o], hr_sem.at[o], sibling)

    def wo_start():
        wo_across(2).start()
        for d, h in SEND_ORDER:
            wo_direct(d, h).start()
        for h in range(n_half):
            wo_handed(0, h).start()
        wo_rest_handed(0).start()

    def wo_spread():
        for o in range(1, x_devs):
            t = column(o)
            remote(wo_share(t), wo_share(t), vs_sem.at[o - 1], vr_sem.at[o - 1], sibling).wait_recv()
        for e in (2, 1, 3):
            for o in range(1, x_devs):
                wo_along(o, e).start()

    all_along = wo_all.at[pl.ds(0, (x_devs - 1) * (cp_devs - 1) * share_rows)]

    for load in loads:
        load.wait()
    with jax.named_scope('a_weights'):
        some_rows = 2 * LANES

        @pl.loop(0, hidden // some_rows)
        def _(i):
            at = pl.ds(pl.multiple_of(i * some_rows, some_rows), some_rows)
            for n in range(3):
                w_in[n, at, :] = w_raw[n, at].reshape(some_rows, w_in.shape[2])

    for step, (b, part, parts) in enumerate(STEPS):
        with jax.named_scope('a_xwait'):
            for o, c, h in BATCHES[b]:
                if c == 0 and o:
                    (onward(h, part) if o == 2 else direct(x_devs - o, h, part)).wait_recv()
                    if (o, h) in ONWARD:
                        onward(h, part).start()
                    handed(o, h, part).start()
            for o, c, h in BATCHES[b]:
                if c == 1:
                    (handed(o, h, part) if o else handed_own(h)).wait_recv()

        if step == len(STEPS) - 2:
            wo_across(1).start()
            wo_across(3).start()
        if step == len(STEPS) - 1:
            wo_start()
        with jax.named_scope('a_qkv'):
            n_rows = half_rows // parts

            @pl.loop(0, 3)
            def _(n):
                x = xg[...] if parts == 1 else x_part[b - 1, part]
                y = jnp.dot(x.reshape(batch_units * n_rows, hidden), w_in[n], preferred_element_type=f32).astype(bf16)
                for i in range(n_heads_loc):
                    for u in range(batch_units):
                        val = y[u * n_rows:(u + 1) * n_rows, i * LANES:(i + 1) * LANES]
                        if parts == 1:
                            stage[i, u, n] = val
                        else:
                            stage_part[b - 1, part, i, u, n] = val

        with jax.named_scope('a_exch'):
            exchange(step)
        with jax.named_scope('a_share'):
            if step >= 2:
                share(step - 2)
        if step == 0:
            with jax.named_scope('a_tables'):
                routing_tables(idx_ref, src_ref, pos_ref, n_dev, local_exp, chunks)
    with jax.named_scope('a_share_last'):
        for step in range(len(STEPS) - 2, len(STEPS)):
            share(step)
    with jax.named_scope('a_wospread'):
        wo_spread()

    with jax.named_scope('a_kvwait'):
        for rr in range(half_cp):
            for step in range(len(STEPS)):
                _, some = rows_of(step)
                got = q_all.at[rr, pl.ds(0, batch_units), some]
                pltpu.make_async_copy(got, got, yq_sem.at[rr, step]).wait()
                got = kv_all.at[(1 - core) * half_cp + rr, pl.ds(0, batch_units), :, some]
                remote(got, got, ks_sem, kr_sem.at[rr, step], sibling).wait_recv()

    scale = LANES ** -0.5 * math.log2(math.e)
    sub_units = half_units // 2
    sub_rows = sub_units * half_rows
    repeat = half_units * half_rows // LANES
    head = col * cp_devs + row

    def scores(q, keys):
        return lax.dot_general(q, keys, (((1,), (1,)), ((), ())), preferred_element_type=f32) * scale

    def lane_sums(p):
        total = p[:, :LANES]
        for i in range(1, p.shape[1] // LANES):
            total += p[:, i * LANES:(i + 1) * LANES]
        return total

    @pl.loop(0, 2 * half_cp)
    def _(turn):
        diagonal = lax.rem(row + col, len(ORDERS))
        piece = pick([pick([order[t] for order in ORDERS], diagonal) for t in range(len(ORDERS))], turn)
        rr, late = piece // 2, lax.rem(piece, 2)
        block = core * half_cp + rr
        place = jnp.where(late == 0, block, 2 * cp_devs - 1 - block)
        with jax.named_scope('a_flash'):
            def queries(sub):
                return q_all[rr, pl.ds(late * half_units + sub * sub_units, sub_units)].reshape(sub_rows, LANES)

            for sub in range(2):
                near = (sub + 1) * sub_units
                keys = kv_all[block, pl.ds(late * half_units, near), 0].reshape(near * half_rows, LANES)
                vals = kv_all[block, pl.ds(late * half_units, near), 1].reshape(near * half_rows, LANES)
                s = scores(queries(sub), keys)
                q_at = sub * sub_rows + lax.broadcasted_iota(jnp.int32, s.shape, 0)
                s = jnp.where(lax.broadcasted_iota(jnp.int32, s.shape, 1) <= q_at, s, -1e30)
                m = jnp.broadcast_to(jnp.max(s, axis=1, keepdims=True), (sub_rows, LANES))
                p = jnp.exp2(s - jnp.concatenate([m] * (s.shape[1] // LANES), axis=1))
                m_run[sub] = m
                l_run[sub] = lane_sums(p)
                acc[sub] = jnp.dot(p.astype(bf16), vals, preferred_element_type=f32)

            @pl.loop(0, place)
            def _(kp):
                k_block = jnp.where(kp < cp_devs, kp, 2 * cp_devs - 1 - kp)
                k_first = jnp.where(kp < cp_devs, 0, half_units)
                keys = kv_all[k_block, pl.ds(k_first, half_units), 0].reshape(half_units * half_rows, LANES)
                vals = kv_all[k_block, pl.ds(k_first, half_units), 1].reshape(half_units * half_rows, LANES)
                both = [scores(queries(sub), keys) for sub in range(2)]
                for sub, s in enumerate(both):
                    before = m_run[sub]
                    m = jnp.maximum(before, jnp.max(s, axis=1, keepdims=True))
                    p = jnp.exp2(s - jnp.concatenate([m] * repeat, axis=1))
                    fade = jnp.exp2(before - m)
                    m_run[sub] = m
                    l_run[sub] = fade * l_run[sub] + lane_sums(p)
                    acc[sub] = fade * acc[sub] + jnp.dot(p.astype(bf16), vals, preferred_element_type=f32)

            for sub in range(2):
                o = acc[sub] / jnp.sum(l_run[sub], axis=1, keepdims=True)
                o_st[rr, pl.ds(late * half_units + sub * sub_units, sub_units)] = o.astype(bf16).reshape(sub_units, half_rows, LANES)

        for t in range(tp_devs // 2):
            to_tp = late * (tp_devs // 2) + t
            src = o_st.at[rr, pl.ds(to_tp * n_half, n_half)]
            own = jnp.logical_and(block == row, to_tp == tp)

            @pl.when(own)
            def _():
                pltpu.make_async_copy(src, og.at[head], or_sem).start()

            @pl.when(jnp.logical_not(own))
            def _():
                remote(src, og.at[head], os_sem, or_sem, {'cp': block, 'tp': to_tp}).start()

        @pl.when(turn == 1)
        def _():
            for o, h in ONWARD:
                wo_from(o, h).wait_recv()
                wo_onward(o, h).start()
                wo_handed(o, h).start()

        @pl.when(turn == 2)
        def _():
            for o, h in ((3, 1), (1, 0)):
                wo_from(o, h).wait_recv()
                wo_handed(o, h).start()

    for h in range(n_half):
        t = column(2)
        remote(wo_part(t, h), wo_part(t, h), wos_sem.at[h], wor_sem.at[h], sibling).wait_recv()
        wo_handed(2, h).start()
    remote(all_along, all_along, us_sem, ur_sem, sibling).wait_recv()
    for o in range(1, x_devs):
        wo_rest_handed(o).start()

    with jax.named_scope('a_owait'):
        pltpu.make_async_copy(og, og, or_sem).wait()
    for n in range(og.shape[0]):
        o_rows[:, n * LANES:(n + 1) * LANES] = og[n].reshape(n_half * half_rows, LANES)
    with jax.named_scope('a_wowait'):
        for o in range(x_devs):
            for h in range(n_half):
                wo_handed(o, h, 1).wait_recv()
            wo_rest_handed(o, 1).wait_recv()

    sub = hidden // LANES
    step = 4 * LANES
    rows = n_half * half_rows

    with jax.named_scope('a_proj'):
        @pl.loop(0, hidden // step)
        def _(j):
            cols = pl.ds(pl.multiple_of(j * step, step), step)
            h = jnp.dot(o_rows[...], wo_all[:, cols], preferred_element_type=f32) + hid_ref[:, :, cols].reshape(rows, step).astype(f32)
            for i in range(step // LANES):
                wide[pl.ds(j * (step // LANES) + i, rows, stride=sub), :] = h[:, i * LANES:(i + 1) * LANES]

    with jax.named_scope('a_rows'):
        @pl.loop(0, rows // 8)
        def _(t):
            for i in range(8):
                h_ref[t * 8 + i] = wide[pl.ds(pl.multiple_of((t * 8 + i) * sub, sub), sub), :].astype(bf16)

    with jax.named_scope('a_drain'):
        for d, h in SEND_ORDER:
            for part in range(2):
                direct(d, h, part).wait_send()
        for o in range(x_devs):
            for h in range(n_half):
                if o:
                    for part in range(2):
                        handed(o, h, part).wait_send()
                else:
                    handed_own(h).wait_send()
                wo_handed(o, h).wait_send()
            wo_rest_handed(o).wait_send()
        for d, h in SEND_ORDER:
            wo_direct(d, h).wait_send()
        for d in range(1, x_devs):
            wo_across(d).wait_send()
        remote(all_along, all_along, us_sem, ur_sem, sibling).wait_send()
        for o, h in ONWARD:
            wo_onward(o, h).wait_send()
            for part in range(2):
                onward(h, part).wait_send()
        for i in range(n_heads_loc):
            @pl.when(core * n_heads_loc + i != row)
            def _():
                remote(q_all.at[0], q_all.at[0], ys_sem.at[0, i], yq_sem.at[0, 0], sibling).wait_send()
                remote(kv_all.at[0], kv_all.at[0], ys_sem.at[1, i], ykv_sem.at[0, 0], sibling).wait_send()
        every = kv_all.at[pl.ds(0, half_cp)]
        remote(every, every, ks_sem, kr_sem.at[0, 0], sibling).wait_send()
        own_row = row // half_cp == core

        @pl.when(own_row)
        def _():
            most = og.at[pl.ds(0, og.shape[0] - 1)]
            remote(most, most, os_sem, or_sem, sibling).wait_send()

        @pl.when(jnp.logical_not(own_row))
        def _():
            remote(og, og, os_sem, or_sem, sibling).wait_send()


def attention_residual(hidden_in, w_query, w_key, w_value, w_out, expert_idx, local_exp, cp_devs, tp_devs, chunks):
    tok_dev, hidden = hidden_in.shape
    heads_loc, head_dim = w_query.shape[1:]
    if w_key.shape != w_query.shape or head_dim != LANES or tp_devs != RING * CORES or heads_loc * CORES != cp_devs:
        raise ValueError('unexpected sizes')
    n_half = 2
    half_rows = tok_dev // n_half
    units = tp_devs * n_half
    n_heads = heads_loc * tp_devs
    batches, batch_units = len(BATCHES), len(BATCHES[0])
    half_cp = cp_devs // 2
    sub = hidden // LANES
    sub_rows = units // 4 * half_rows
    bf16, f32 = jnp.bfloat16, jnp.float32
    dma = pltpu.SemaphoreType.DMA
    n_dev = cp_devs * tp_devs
    return pl.pallas_call(
        functools.partial(attention_kernel, cp_devs, tp_devs, local_exp, chunks),
        out_shape=[jax.ShapeDtypeStruct((tok_dev, sub, LANES), bf16), jax.ShapeDtypeStruct((n_dev, LANES), jnp.int32),
                   jax.ShapeDtypeStruct(expert_idx.shape[::-1], jnp.int32)],
        in_specs=[pl.BlockSpec(memory_space=pltpu.VMEM)] + [pl.BlockSpec(memory_space=pl.ANY)] * 4 + [pl.BlockSpec(memory_space=pltpu.VMEM)],
        out_specs=[pl.BlockSpec(memory_space=pltpu.VMEM)] * 3,
        scratch_shapes=[
            pltpu.VMEM((3, hidden, heads_loc, head_dim), bf16),
            pltpu.VMEM((3, hidden, heads_loc * head_dim), bf16),
            pltpu.VMEM((batch_units, half_rows, hidden), bf16),
            pltpu.VMEM((batches - 1, 2, batch_units, half_rows // 2, hidden), bf16),
            pltpu.VMEM((heads_loc, batch_units, 3, half_rows, LANES), bf16),
            pltpu.VMEM((batches - 1, 2, heads_loc, batch_units, 3, half_rows // 2, LANES), bf16),
            pltpu.VMEM((half_cp, units, half_rows, LANES), bf16),
            pltpu.VMEM((cp_devs, units, 2, half_rows, LANES), bf16),
            pltpu.VMEM((half_cp, units, half_rows, LANES), bf16),
            pltpu.VMEM((n_heads, n_half, half_rows, LANES), bf16),
            pltpu.VMEM((tok_dev, hidden), bf16),
            pltpu.VMEM((n_heads * head_dim, hidden), bf16),
            pltpu.VMEM((tok_dev * sub, LANES), f32),
            pltpu.VMEM((2, sub_rows, LANES), f32),
            pltpu.VMEM((2, sub_rows, LANES), f32),
            pltpu.VMEM((2, sub_rows, LANES), f32),
            dma((RING - 1, n_half, 2)), dma((RING - 1, n_half, 2)), dma((RING, n_half, 2)), dma((RING, n_half, 2)),
            dma((n_half, 2)), dma((n_half, 2)),
            dma((2, heads_loc)), dma((half_cp, len(STEPS))), dma((half_cp, len(STEPS))), dma, dma((half_cp, len(STEPS))),
            dma((RING - 1, n_half)), dma((RING - 1, n_half)), dma((RING, n_half)), dma((RING, n_half)), dma((2,)), dma((2,)),
            dma((RING - 1,)), dma((RING - 1,)), dma, dma, dma((RING,)), dma((RING,)), dma, dma, dma((4,)),
        ],
        compiler_params=pltpu.CompilerParams(collective_id=1, has_side_effects=True, vmem_limit_bytes=67043328),
        cost_estimate=pl.CostEstimate(flops=12 * 10 ** 9, bytes_accessed=16 * 10 ** 6, transcendentals=10 ** 7),
        name='attention_exchange',
    )(hidden_in.reshape(n_half, half_rows, hidden), w_query, w_key, w_value, w_out.reshape(heads_loc * head_dim, hidden), expert_idx.T)


from jax.sharding import PartitionSpec as P


def solution(mesh):
    cp_devs, tp_devs = mesh.shape['cp'], mesh.shape['tp']
    row_spec = P(('dp', 'cp', 'tp'), None)
    head_spec = P(None, 'tp', None)
    expert_spec = P(('cp', 'tp'), None, None)

    def device_step(hidden_in, w_query, w_key, w_value, w_out, expert_idx, gate_vals, w_gate, w_up, w_down):
        chunks = 3
        h_tiles, src, pos = attention_residual(hidden_in, w_query, w_key, w_value, w_out, expert_idx, w_gate.shape[0], cp_devs, tp_devs, chunks)
        return moe(h_tiles, src, pos, gate_vals, w_gate, w_up, w_down, cp_devs, tp_devs, chunks)

    return jax.shard_map(device_step, mesh=mesh, in_specs=(row_spec, head_spec, head_spec, head_spec, P('tp', None, None), row_spec, row_spec, expert_spec, expert_spec, expert_spec), out_specs=row_spec, check_vma=False)
```
